32 devices in a mesh: intv: 1, node: 4 (over y, x), row: 8 (over z, core).
Axes of the slice: x: 2, y: 2, z: 4, core: 2. Of those that a mesh axis runs over, the one named last changes fastest.
Arguments:
- inv_factors: float32 [4, 8, 2, 512, 512], P(('intv', 'node'), 'row'), may hold values from -0.48535534 to 0.48535534, as said below
- coupling: float32 [8, 512, 512], P('row'), may hold values from -0.5 to 0.5
- vectors: float32 [8, 512, 64], P('row'), may hold values from -6 to 6
Outputs:
- moments: float32 [8, 512, 256], P(('intv', 'row'), 'node')
- gram: float32 [256, 256], P('intv')
The draws below stay inside these ranges and needn't reach their ends.
Inputs may be any that keep to these rules, and one draw needn't show every extreme that they name: `inv_factors`: each [j, k] entry holds the real part then the imaginary part of a full 512 x 512 inverse factor.
All inputs are finite; a program needn't handle non-finite values.
Results may differ from the reference program's by a relative error of at most 0.0003.
Values sent between devices are 32-bit elements; how exact they have to be, the bound alone decides.
No kernel may reach another device: no remote copies, remote signals or barrier semaphores. Data moves between devices by JAX's collectives and lax.ppermute only.
A program may use at most 64 MiB of HBM per device.

```python
import functools
import math
import jax
import jax.numpy as jnp
from jax import lax

BS = 512
NVEC = 64
MOM = 2
NB = 8
NQ = 4
NROWS = 4096
COLS = 256


def draw_inv_factors(key, part):
    key_off, key_mag, key_phase = jax.random.split(jax.random.fold_in(key, 17), 3)
    spread = 0.2 / math.sqrt(BS)
    offdiag = jax.random.truncated_normal(key_off, -4.0, 4.0, (NQ, NB, 2, BS, BS), jnp.float32) * spread
    magnitude = jax.random.uniform(key_mag, (NQ, NB, 1, BS), jnp.float32, 0.2, 0.45)
    phase = jax.random.uniform(key_phase, (NQ, NB, 1, BS), jnp.float32, -math.pi, math.pi)
    diagonal = jnp.concatenate([magnitude * jnp.cos(phase), magnitude * jnp.sin(phase)], axis=2)
    identity = jnp.eye(BS, dtype=jnp.float32)
    return offdiag + diagonal[..., None] * identity


def block_scale(stream_key, shape, cuts, low, top_value):
    loudness = 1.0
    for position, blocks in cuts:
        steps = jax.random.uniform(jax.random.fold_in(jax.random.fold_in(stream_key, 6), position), (blocks,), jnp.float32, low / len(cuts), top_value / len(cuts))
        loudness = loudness * jnp.repeat(jnp.exp(steps), shape[position] // blocks).reshape((-1,) + (1,) * (len(shape) - 1 - position))
    return loudness


def normal_values(own_key, shape, scale, limit, cuts=(), held_as=jnp.bfloat16):
    level = block_scale(own_key, shape, cuts, -0.22, 0.18) if cuts else 1.0
    entries = jax.random.normal(own_key, shape, jnp.float32) * scale * level
    return jnp.minimum(jnp.maximum(entries, -limit), limit).astype(held_as)


def setup_inputs(seed: int = 0, part: int = 0) -> dict:
    streams_of = jax.random.split(jax.random.key(seed), 4)
    part_keys = jax.random.split(jax.random.fold_in(streams_of[3], part), 4)
    inv_factors = draw_inv_factors(jax.random.fold_in(jax.random.fold_in(streams_of[3], part), 71), part)
    coupling = normal_values(streams_of[1], (NB, BS, BS), (BS // 4) ** -0.5, 0.5, ((0, 8),), jnp.float32)
    vectors = normal_values(streams_of[2], (NB, BS, NVEC), 1.0, 6.0, ((0, 8),), jnp.float32)
    return {"inv_factors": inv_factors, "coupling": coupling, "vectors": vectors}


HIGH = lax.Precision.HIGHEST


def complex_product(factor, block):
    half = block.shape[1] // 2
    real_side = jnp.dot(factor[0], block, precision=HIGH)
    imag_side = jnp.dot(factor[1], block, precision=HIGH)
    return jnp.concatenate([real_side[:, :half] - imag_side[:, half:], real_side[:, half:] + imag_side[:, :half]], axis=1)


def solve_node(factors, coupling, vectors):
    filler = jnp.zeros((BS, NVEC), jnp.float32)
    carry = jnp.zeros((BS, 2 * NVEC), jnp.float32)
    forward = []
    for block_id in range(NB):
        start = jnp.concatenate([vectors[block_id], filler], axis=1) + carry
        upper = complex_product(factors[block_id], start)
        forward.append(upper)
        carry = jnp.dot(coupling[block_id].T, upper, precision=HIGH)
    solved = [None] * NB
    solved[NB - 1] = forward[NB - 1]
    for block_id in range(NB - 2, -1, -1):
        coupled = jnp.dot(coupling[block_id], solved[block_id + 1], precision=HIGH)
        solved[block_id] = forward[block_id] + complex_product(factors[block_id], coupled)
    return jnp.stack(solved)


def reference(inv_factors, coupling, vectors):
    solver = functools.partial(solve_node, coupling=coupling, vectors=vectors)
    solutions = lax.map(solver, inv_factors)
    nodes_index = jnp.arange(NQ).astype(jnp.float32)
    theta = 2.0 * math.pi * (nodes_index + 0.5) / NQ
    real_sol = solutions[..., :NVEC]
    imag_sol = solutions[..., NVEC:]
    pieces = []
    for order in range(MOM):
        w_real = jnp.cos((order + 1) * theta) / NQ
        w_imag = jnp.sin((order + 1) * theta) / NQ
        pieces.append(jnp.einsum('q,qbrc->brc', w_real, real_sol) - jnp.einsum('q,qbrc->brc', w_imag, imag_sol))
        pieces.append(jnp.einsum('q,qbrc->brc', w_real, imag_sol) + jnp.einsum('q,qbrc->brc', w_imag, real_sol))
    moments = jnp.concatenate(pieces, axis=-1)
    flat = moments.reshape(NROWS, COLS)
    gram = jnp.einsum('rc,rd->cd', flat, flat, precision=HIGH) * (NQ / NROWS)
    return moments, gram
```

```python
import math

import jax
import jax.numpy as jnp
from jax import lax
from jax.sharding import PartitionSpec as P

MOM = 2
PREC = lax.Precision.HIGH


def dot_nt(rows, matrix):
    return lax.dot_general(rows, matrix, (((1,), (1,)), ((), ())), precision=PREC)


def apply_t(matrix, rows):
    n = matrix.shape[1]
    w = rows.shape[0] // 2
    q = dot_nt(rows, matrix)
    return jnp.concatenate([q[:w, :n] - q[w:, n:], q[:w, n:] + q[w:, :n]], axis=0)


def product(left, right):
    n = left.shape[1]
    q_re = jnp.dot(left, right[:n], precision=PREC)
    q_im = jnp.dot(left, right[n:], precision=PREC)
    return jnp.concatenate([q_re[:n] - q_im[n:], q_re[n:] + q_im[:n]], axis=0)


def tree_sum(values):
    while len(values) > 1:
        values = [values[i] + values[i + 1] for i in range(0, len(values), 2)]
    return values[0]


def shards(inv_factors, coupling, vectors):
    n = inv_factors.shape[3]
    width = vectors.shape[2]
    half = width // 2
    rows = lax.axis_size("row")
    nodes = lax.axis_size("node")
    layers = rows // 2
    core = lax.axis_index("row") % 2
    layer = lax.axis_index("row") // 2
    node = lax.axis_index("node")
    first = core == 0

    def swap_core(value):
        return lax.ppermute(value, "row", [(r, r ^ 1) for r in range(rows)])

    def hop(value, source, target):
        return lax.ppermute(value, "row", [(2 * source + c, 2 * target + c) for c in range(2)])

    def exchange_node(value, d):
        return lax.ppermute(value, "node", [(j, j ^ d) for j in range(nodes)])

    def exchange_layer(value, d):
        return lax.ppermute(value, "row", [(r, r ^ (2 * d)) for r in range(rows)])

    factor = inv_factors[0, 0].reshape(2 * n, n)
    couple = coupling[0]
    v_t = vectors[0].T

    q = dot_nt(v_t, factor)
    own_u = jnp.concatenate([q[:, :n], q[:, n:]], axis=0)
    own_c = jnp.dot(own_u, couple, precision=PREC)
    from_a = swap_core(own_c)
    y = jnp.concatenate([v_t + from_a[:width], from_a[width:]], axis=0)
    w_full = jnp.dot(apply_t(factor, y), couple, precision=PREC)
    w_lo = jnp.concatenate([w_full[:half], w_full[width : width + half]], axis=0)
    w_hi = jnp.concatenate([w_full[half:width], w_full[width + half :]], axis=0)
    w_loc = jnp.where(first, swap_core(w_lo), w_hi)

    a_own = jnp.concatenate(
        [
            lax.dot_general(couple, factor[:n], (((0,), (0,)), ((), ())), precision=PREC),
            lax.dot_general(couple, factor[n:], (((0,), (0,)), ((), ())), precision=PREC),
        ],
        axis=0,
    )
    a_other = swap_core(a_own)
    a_a = jnp.where(first, a_own, a_other)
    a_b = jnp.where(first, a_other, a_own)
    p_mat = product(a_b, a_a)
    b_own = jnp.dot(factor, couple, precision=PREC)
    b_other = swap_core(b_own)
    b_a = jnp.where(first, b_own, b_other)
    b_b = jnp.where(first, b_other, b_own)
    q_mat = product(b_a, b_b)
    f_other = swap_core(factor)
    f_a = jnp.where(first, factor, f_other)
    f_b = jnp.where(first, f_other, factor)
    v_other = swap_core(v_t)
    v_a = jnp.where(first, v_t, v_other)
    v_b = jnp.where(first, v_other, v_t)
    zero = jnp.zeros((half, n), jnp.float32)
    va_half = jnp.concatenate([jnp.where(first, v_a[:half], v_a[half:]), zero], axis=0)
    vb_half = jnp.concatenate([jnp.where(first, v_b[:half], v_b[half:]), zero], axis=0)

    carry = jnp.zeros((2 * half, n), jnp.float32)
    leaving = w_loc
    for t in range(layers - 1):
        got = hop(leaving, t, t + 1)
        carry = carry + got
        if t < layers - 2:
            leaving = w_loc + apply_t(p_mat, got)
    y_a = va_half + carry
    u_a = apply_t(f_a, y_a)
    u_b = apply_t(f_b, vb_half + apply_t(a_a, y_a))
    s_loc = u_a + apply_t(b_a, u_b)

    following = jnp.zeros((2 * half, n), jnp.float32)
    leaving = s_loc
    for t in range(layers - 1, 0, -1):
        got = hop(leaving, t, t - 1)
        following = following + got
        if t > 1:
            leaving = s_loc + apply_t(q_mat, got)
    x_a = s_loc + apply_t(q_mat, following)
    x_b = u_b + apply_t(b_b, following)

    keep = jnp.where(first, x_a, x_b)
    recv = swap_core(jnp.where(first, x_b, x_a))
    lo = jnp.where(first, keep, recv)
    hi = jnp.where(first, recv, keep)
    x_own = jnp.concatenate([lo[:half], hi[:half], lo[half:], hi[half:]], axis=0).T

    share = n // nodes
    pieces = [lax.dynamic_slice_in_dim(x_own, (node ^ d) * share, share, 0) for d in range(nodes)]
    blocks = [pieces[0]] + [exchange_node(pieces[d], d) for d in range(1, nodes)]
    parts = []
    for order in range(MOM):
        re_terms, im_terms = [], []
        for d in range(nodes):
            theta = 2.0 * math.pi * ((node ^ d).astype(jnp.float32) + 0.5) / nodes
            w_re = jnp.cos((order + 1) * theta) / nodes
            w_im = jnp.sin((order + 1) * theta) / nodes
            re, im = blocks[d][:, :width], blocks[d][:, width:]
            re_terms.append(w_re * re - w_im * im)
            im_terms.append(w_re * im + w_im * re)
        parts += [tree_sum(re_terms), tree_sum(im_terms)]
    moments = jnp.concatenate(parts, axis=1)
    cols = moments.shape[1]

    gram = lax.dot_general(moments, moments, (((0,), (0,)), ((), ())), precision=PREC)
    hc = cols // 2
    top, bottom = gram[:hc], gram[hc:]
    mine = jnp.where(first, top, bottom) + swap_core(jnp.where(first, bottom, top))
    gs = hc // nodes
    own = [lax.dynamic_slice_in_dim(mine, (node ^ d) * gs, gs, 0) for d in range(nodes)]
    piece = tree_sum([own[0]] + [exchange_node(own[d], d) for d in range(1, nodes)])
    piece = tree_sum([piece] + [exchange_layer(piece, d) for d in range(1, layers)])
    piece = piece * (nodes / (rows * n))
    got = [piece] + [exchange_node(piece, d) for d in range(1, nodes)]
    mine = jnp.zeros((hc, cols), jnp.float32)
    for d in range(nodes):
        mine = lax.dynamic_update_slice_in_dim(mine, got[d], (node ^ d) * gs, 0)
    other = swap_core(mine)
    gram = jnp.concatenate([jnp.where(first, mine, other), jnp.where(first, other, mine)], axis=0)
    return moments[None], gram


def solution(mesh):
    return jax.shard_map(
        shards,
        mesh=mesh,
        in_specs=(
            P(("intv", "node"), "row", None, None, None),
            P("row", None, None),
            P("row", None, None),
        ),
        out_specs=(P(("intv", "row"), "node", None), P("intv", None)),
        check_vma=False,
    )
```

```python
import functools
import functools
import math

import jax
import jax.numpy as jnp
from jax import lax
from jax.experimental import pallas as pl
from jax.experimental.pallas import tpu as pltpu
from jax.sharding import PartitionSpec as P


MOM = 2
PREC = lax.Precision.HIGH
F32, BF16 = jnp.float32, jnp.bfloat16
NN = (((1,), (0,)), ((), ()))
NT = (((1,), (1,)), ((), ()))
VMEM = pl.BlockSpec(memory_space=pltpu.VMEM)
HBM = pl.BlockSpec(memory_space=pltpu.HBM)
CHUNKS = 4


def parts_of(x):
    high = x.astype(BF16)
    return high, (x - high.astype(F32)).astype(BF16)


def times(rows, matrix, dims):
    w = rows.shape[0]
    high, low = parts_of(rows)
    both = lax.dot_general(
        jnp.concatenate([high, low], axis=0), matrix[0], dims, preferred_element_type=F32
    )
    rest = lax.dot_general(high, matrix[1], dims, preferred_element_type=F32)
    return both[:w] + (both[w:] + rest)


def apply_to(rows, matrix):
    w, n = rows.shape[0] // 2, rows.shape[1]
    q = times(rows, matrix, NT)
    return jnp.concatenate([q[:w, :n] - q[w:, n:], q[:w, n:] + q[w:, :n]], axis=0)


def add_real(block, real):
    w = real.shape[0]
    return jnp.concatenate([block[:w] + real, block[w:]], axis=0)


def read(pair):
    return pair[0][...], pair[1][...]


def block_of(pair, role):
    return pair[0][role], pair[1][role]


def write(pair, value):
    high, low = parts_of(value)
    pair[0][...] = high
    pair[1][...] = low


def call(kernel, outs, *operands):
    return pl.pallas_call(
        kernel,
        out_shape=tuple(pltpu.VMEM(shape, dtype) for shape, dtype in outs),
        in_specs=[VMEM] * len(operands),
        out_specs=tuple([VMEM] * len(outs)),
        compiler_params=pltpu.CompilerParams(vmem_limit_bytes=20 << 20),
    )(*[pltpu.with_memory_space_constraint(x, pltpu.VMEM) for x in operands])


def enter_kernel(f_any, c_any, v_any, fh, fl, ch, cl, vt, g, f_buf, c_buf, v_buf, sems):
    n = c_buf.shape[0]
    rows = f_buf.shape[0] // CHUNKS
    v_copy = pltpu.make_async_copy(v_any, v_buf, sems.at[CHUNKS])
    v_copy.start()
    copies = []
    for i in range(CHUNKS):
        part = pl.ds(i * rows, rows)
        copies.append(pltpu.make_async_copy(f_any.at[part], f_buf.at[part], sems.at[i]))
        copies[-1].start()
    c_copy = pltpu.make_async_copy(c_any, c_buf, sems.at[CHUNKS + 1])
    c_copy.start()
    v_copy.wait()
    real = v_buf[...]
    vt[...] = real
    pieces = []
    for i in range(CHUNKS):
        part = pl.ds(i * rows, rows)
        copies[i].wait()
        high, low = parts_of(f_buf[part, :])
        fh[part, :] = high
        fl[part, :] = low
        pieces.append(times(real, (high, low), NT))
    q = jnp.concatenate(pieces, axis=1)
    u = jnp.concatenate([q[:, :n], q[:, n:]], axis=0)
    c_copy.wait()
    write((ch, cl), c_buf[...])
    g[...] = times(u, read((ch, cl)), NN)


def leave_kernel(vt, g, fh, fl, ch, cl, lo, hi):
    y = add_real(g[...], vt[...])
    w = times(apply_to(y, read((fh, fl))), read((ch, cl)), NN)
    half = lo.shape[0] // 2
    width = 2 * half
    lo[...] = jnp.concatenate([w[:half], w[width : width + half]], axis=0)
    hi[...] = jnp.concatenate([w[half:width], w[width + half :]], axis=0)


def pair_product(left, right, dims):
    return lax.dot_general(left[0], right[0], dims, preferred_element_type=F32) + (
        lax.dot_general(left[0], right[1], dims, preferred_element_type=F32)
        + lax.dot_general(left[1], right[0], dims, preferred_element_type=F32)
    )


def product_kernel(compute, *refs):
    operands, (whole, buf, sem) = refs[:-3], refs[-3:]
    buf[...] = compute(*operands)
    copy = pltpu.make_async_copy(buf, whole, sem)
    copy.start()
    copy.wait()


def product_in_place(compute, *refs):
    refs[-1][...] = compute(*refs[:-1])


def product(compute, shape, *operands):
    return pl.pallas_call(
        functools.partial(product_kernel, compute),
        out_shape=pltpu.HBM(shape, F32),
        in_specs=[VMEM] * len(operands),
        out_specs=HBM,
        scratch_shapes=[pltpu.VMEM(shape, F32), pltpu.SemaphoreType.DMA(())],
        compiler_params=pltpu.CompilerParams(vmem_limit_bytes=20 << 20),
    )(*[pltpu.with_memory_space_constraint(x, pltpu.VMEM) for x in operands])


def a_part(index, fh, fl, ch, cl):
    n = ch.shape[0]
    part = pl.ds(index * n, n)
    return pair_product((ch[...].T, cl[...].T), (fh[part, :], fl[part, :]), NN)


def b_part(fh, fl, ch, cl):
    return pair_product(read((fh, fl)), read((ch, cl)), NN)


def roles_kernel(count, *refs):
    sources = (refs[:count], refs[count : 2 * count])
    high, low, buf, sems = refs[-4:]
    mine = lax.axis_index("row") % 2
    slots = (mine, 1 - mine)
    rows = buf.shape[1] // CHUNKS
    copies = []
    for side in range(2):
        start = 0
        for source in sources[side]:
            for i in range(source.shape[0] // rows):
                copy = pltpu.make_async_copy(
                    source.at[pl.ds(i * rows, rows)],
                    buf.at[side, pl.ds(start, rows)],
                    sems.at[side, start // rows],
                )
                copy.start()
                copies.append((side, start, copy))
                start += rows
    for side, start, copy in copies:
        copy.wait()
        part = pl.ds(start, rows)
        h, l = parts_of(buf[side, part, :])
        high[slots[side], part, :] = h
        low[slots[side], part, :] = l


def roles_and_vectors_kernel(count, *refs):
    v_own, v_other, va, vb = refs[2 * count : 2 * count + 4]
    roles_kernel(count, *refs[: 2 * count], *refs[-4:])
    mine = lax.axis_index("row") % 2
    half = va.shape[0]
    own = v_own[pl.ds(pl.multiple_of(mine * half, half), half), :]
    other = v_other[pl.ds(pl.multiple_of(mine * half, half), half), :]
    va[...] = jnp.where(mine == 0, own, other)
    vb[...] = jnp.where(mine == 0, other, own)


def roles(owns, others, vectors=()):
    n = others[0].shape[1]
    shape = (2, 2 * n, n)
    halves = [(v.shape[0] // 2, n) for v in vectors]
    body = roles_and_vectors_kernel if vectors else roles_kernel
    return pl.pallas_call(
        functools.partial(body, len(others)),
        out_shape=tuple(pltpu.VMEM(half, F32) for half in halves)
        + (pltpu.VMEM(shape, BF16), pltpu.VMEM(shape, BF16)),
        in_specs=[HBM] * (2 * len(others)) + [VMEM] * len(vectors),
        out_specs=(VMEM,) * (2 + len(halves)),
        scratch_shapes=[pltpu.VMEM(shape, F32), pltpu.SemaphoreType.DMA((2, CHUNKS))],
        compiler_params=pltpu.CompilerParams(vmem_limit_bytes=20 << 20),
    )(
        *[pltpu.with_memory_space_constraint(x, pltpu.HBM) for x in owns],
        *others,
        *[pltpu.with_memory_space_constraint(x, pltpu.VMEM) for x in vectors],
    )


def forward_kernel(*refs):
    *cs, va, vb, ah, al, out = refs
    c = cs[0][...]
    for other in cs[1:]:
        c = c + other[...]
    y = apply_to(add_real(c, va[...]), block_of((ah, al), 0))
    out[...] = apply_to(add_real(y, vb[...]), block_of((ah, al), 1))


def turn_kernel(c, va, vb, fh, fl, ah, al, bh, bl, ua, ub, s):
    y = add_real(c[...], va[...])
    y_b = add_real(apply_to(y, block_of((ah, al), 0)), vb[...])
    u_b = apply_to(y_b, block_of((fh, fl), 1))
    u_a = apply_to(y, block_of((fh, fl), 0))
    ub[...] = u_b
    ua[...] = u_a
    s[...] = u_a + apply_to(u_b, block_of((bh, bl), 0))


def backward_kernel(r, ua, ub, bh, bl, xa, *xb):
    x_b = ub[...] + apply_to(r[...], block_of((bh, bl), 1))
    for out in xb:
        out[...] = x_b
    xa[...] = ua[...] + apply_to(x_b, block_of((bh, bl), 0))


def after(*values, every=False):
    held = lax.optimization_barrier(values)
    return held if every else held[0]


def tree_sum(values):
    while len(values) > 1:
        values = [values[i] + values[i + 1] for i in range(0, len(values), 2)]
    return values[0]


def shards(inv_factors, coupling, vectors):
    n = inv_factors.shape[3]
    width = vectors.shape[2]
    half = width // 2
    rows = lax.axis_size("row")
    nodes = lax.axis_size("node")
    layers = rows // 2
    core = lax.axis_index("row") % 2
    node = lax.axis_index("node")
    first = core == 0

    def swap_core(value):
        return lax.ppermute(value, "row", [(r, r ^ 1) for r in range(rows)])

    def hop(value, source, target):
        return lax.ppermute(value, "row", [(2 * source + c, 2 * target + c) for c in range(2)])

    def exchange_node(value, d):
        return lax.ppermute(value, "node", [(j, j ^ d) for j in range(nodes)])

    def exchange_layer(value, d):
        return lax.ppermute(value, "row", [(r, r ^ (2 * d)) for r in range(rows)])

    factor = inv_factors[0, 0].reshape(2 * n, n)
    couple = coupling[0]
    block = ((2 * half, n), F32)

    fh, fl, ch, cl, v_t, g = pl.pallas_call(
        enter_kernel,
        out_shape=(
            pltpu.VMEM((2 * n, n), BF16),
            pltpu.VMEM((2 * n, n), BF16),
            pltpu.VMEM((n, n), BF16),
            pltpu.VMEM((n, n), BF16),
            pltpu.VMEM((width, n), F32),
            pltpu.VMEM((2 * width, n), F32),
        ),
        in_specs=[HBM] * 3,
        out_specs=(VMEM,) * 6,
        scratch_shapes=[
            pltpu.VMEM((2 * n, n), F32),
            pltpu.VMEM((n, n), F32),
            pltpu.VMEM((width, n), F32),
            pltpu.SemaphoreType.DMA((CHUNKS + 2,)),
        ],
        compiler_params=pltpu.CompilerParams(vmem_limit_bytes=20 << 20),
        name="enter",
    )(*[pltpu.with_memory_space_constraint(x, pltpu.HBM) for x in (factor, couple, vectors[0].T)])
    from_a = swap_core(g)
    (a_re,) = call(
        functools.partial(product_in_place, functools.partial(a_part, 0)),
        [((n, n), F32)], after(fh, g), fl, ch, cl,
    )
    lo, hi = call(leave_kernel, [block, block], v_t, from_a, after(fh, from_a), fl, ch, cl)

    got_lo = lax.ppermute(lo, "row", [(1, 2)])
    got_hi = lax.ppermute(hi, "row", [(1, 3)])
    got = [got_lo, got_hi]
    a_im = product(functools.partial(a_part, 1), (n, n), after(fh, lo), fl, ch, cl)
    a_re_other = swap_core(after(a_re, lo))
    a_im_other = swap_core(a_im)
    v_other = swap_core(after(v_t, lo))
    va, vb, *a_mats = roles([a_re, a_im], [a_re_other, a_im_other], [v_t, v_other])
    f_other = swap_core(after(factor, a_re_other, a_im_other))
    carry = jnp.zeros((2 * half, n), F32)
    for t in range(layers - 1):
        if t > 0:
            got = [hop(leaving, t, t + 1)]
        carry = sum(got, carry)
        if t < layers - 2:
            (leaving,) = call(forward_kernel, [block], *got, va, vb, *a_mats)
        if t == 0:
            f_mats = roles([after(factor, leaving)], [f_other])
            b_own = product(b_part, (2 * n, n), after(fh, leaving), fl, ch, cl)
            b_other = swap_core(b_own)
        if t == 1:
            b_mats = roles([after(b_own, leaving)], [b_other])
    u_a, u_b, leaving = call(turn_kernel, [block] * 3, carry, va, vb, *f_mats, *a_mats, *b_mats)

    following = jnp.zeros((2 * half, n), F32)
    for t in range(layers - 1, 0, -1):
        got = hop(leaving, t, t - 1)
        following = following + got
        if t > 1:
            (leaving,) = call(backward_kernel, [block], got, u_a, u_b, *b_mats)
    x_a, x_b = call(backward_kernel, [block] * 2, following, u_a, u_b, *b_mats)

    share = n // nodes
    x_both = jnp.concatenate([x_a, x_b], axis=0)
    pieces = [lax.dynamic_slice_in_dim(x_both, (node ^ d) * share, share, 1) for d in range(nodes)]
    pieces = [pieces[0]] + [exchange_node(pieces[d], d) for d in range(1, nodes)]
    pieces = [p.reshape(2, 2, half, share) for p in pieces]
    terms = []
    for order in range(MOM):
        re_terms, im_terms = [], []
        for d in range(nodes):
            theta = 2.0 * math.pi * ((node ^ d).astype(F32) + 0.5) / nodes
            w_re = jnp.cos((order + 1) * theta) / nodes
            w_im = jnp.sin((order + 1) * theta) / nodes
            re, im = pieces[d][:, 0], pieces[d][:, 1]
            re_terms.append(w_re * re - w_im * im)
            im_terms.append(w_re * im + w_im * re)
        terms += [tree_sum(re_terms), tree_sum(im_terms)]
    mine = jnp.stack(terms, axis=1)
    groups = 2 * MOM
    cols = groups * width
    other = swap_core(mine.reshape(2 * groups * half, share)).reshape(mine.shape)
    both = jnp.stack([jnp.where(first, mine, other), jnp.where(first, other, mine)], axis=2)
    both = both.reshape(2, cols, share)
    moments = jnp.where(first, both[0], both[1])

    mine = mine.reshape(2, groups * half, share)
    gram = lax.dot_general(mine[0], both[0], NT, precision=PREC) + lax.dot_general(
        mine[1], both[1], NT, precision=PREC
    )
    hc = groups * half
    layer = lax.axis_index("row") // 2
    gs = hc // layers
    own = [lax.dynamic_slice_in_dim(gram, (layer ^ d) * gs, gs, 0) for d in range(layers)]
    piece = tree_sum([own[0]] + [exchange_layer(own[d], d) for d in range(1, layers)])
    piece = tree_sum([piece] + [exchange_node(piece, d) for d in range(1, nodes)])
    piece = piece * (nodes / (rows * n))
    got = [piece] + [exchange_layer(piece, d) for d in range(1, layers)]
    gram = jnp.zeros((hc, cols), F32)
    for d in range(layers):
        gram = lax.dynamic_update_slice_in_dim(gram, got[d], (layer ^ d) * gs, 0)
    other = swap_core(gram)
    gram = gram.reshape(groups, half, cols)
    other = other.reshape(groups, half, cols)
    gram = jnp.stack([jnp.where(first, gram, other), jnp.where(first, other, gram)], axis=1)
    return moments.T[None], gram.reshape(cols, cols)


def solution(mesh):
    return jax.shard_map(
        shards,
        mesh=mesh,
        in_specs=(
            P(("intv", "node"), "row", None, None, None),
            P("row", None, None),
            P("row", None, None),
        ),
        out_specs=(P(("intv", "row"), "node", None), P("intv", None)),
        check_vma=False,
    )
```

```python
import functools
import functools
import math

import jax
import jax.numpy as jnp
from jax import lax
from jax.experimental import pallas as pl
from jax.experimental.pallas import tpu as pltpu
from jax.sharding import PartitionSpec as P


MOM = 2
PREC = lax.Precision.HIGH
F32, BF16 = jnp.float32, jnp.bfloat16
NN = (((1,), (0,)), ((), ()))
NT = (((1,), (1,)), ((), ()))
VMEM = pl.BlockSpec(memory_space=pltpu.VMEM)
HBM = pl.BlockSpec(memory_space=pltpu.HBM)
CHUNKS = 4


def parts_of(x):
    high = x.astype(BF16)
    return high, (x - high.astype(F32)).astype(BF16)


def times(rows, matrix, dims):
    w = rows.shape[0]
    high, low = parts_of(rows)
    both = lax.dot_general(
        jnp.concatenate([high, low], axis=0), matrix[0], dims, preferred_element_type=F32
    )
    rest = lax.dot_general(high, matrix[1], dims, preferred_element_type=F32)
    return both[:w] + (both[w:] + rest)


def apply_to(rows, matrix, dims):
    w = rows.shape[0] // 2
    re, im = (times(rows, part, dims) for part in matrix)
    return jnp.concatenate([re[:w] - im[w:], im[:w] + re[w:]], axis=0)


def add_real(block, real):
    w = real.shape[0]
    return jnp.concatenate([block[:w] + real, block[w:]], axis=0)


def read(pair):
    return pair[0][...], pair[1][...]


def block_of(pair, *role):
    return tuple((pair[0][(*role, part)], pair[1][(*role, part)]) for part in range(2))


def write(pair, value):
    high, low = parts_of(value)
    pair[0][...] = high
    pair[1][...] = low


def call(kernel, outs, *operands):
    return pl.pallas_call(
        kernel,
        out_shape=tuple(pltpu.VMEM(shape, dtype) for shape, dtype in outs),
        in_specs=[VMEM] * len(operands),
        out_specs=tuple([VMEM] * len(outs)),
        compiler_params=pltpu.CompilerParams(vmem_limit_bytes=20 << 20),
    )(*[pltpu.with_memory_space_constraint(x, pltpu.VMEM) for x in operands])


def enter_kernel(f_any, c_any, v_any, fh, fl, ch, cl, vt, g, f_buf, c_buf, v_buf, sems):
    n = c_buf.shape[0]
    per_part = CHUNKS // 2
    rows = n // per_part
    v_copy = pltpu.make_async_copy(v_any, v_buf, sems.at[CHUNKS])
    v_copy.start()
    copies = []
    places = [(i // per_part, pl.ds(i % per_part * rows, rows)) for i in range(CHUNKS)]
    for i, place in enumerate(places):
        copies.append(pltpu.make_async_copy(f_any.at[place], f_buf.at[place], sems.at[i]))
        copies[-1].start()
    c_copy = pltpu.make_async_copy(c_any, c_buf, sems.at[CHUNKS + 1])
    c_copy.start()
    v_copy.wait()
    real = v_buf[...]
    vt[...] = real
    pieces = []
    for copy, place in zip(copies, places):
        copy.wait()
        high, low = parts_of(f_buf[place])
        fh[place] = high
        fl[place] = low
        pieces.append(times(real, (high, low), NT))
    q = jnp.concatenate(pieces, axis=1)
    u = jnp.concatenate([q[:, :n], q[:, n:]], axis=0)
    c_copy.wait()
    write((ch, cl), c_buf[...])
    g[...] = times(u, read((ch, cl)), NN)


def leave_kernel(vt, g, fh, fl, ch, cl, lo, hi):
    y = add_real(g[...], vt[...])
    w = times(apply_to(y, block_of((fh, fl)), NT), read((ch, cl)), NN)
    half = lo.shape[0] // 2
    width = 2 * half
    lo[...] = jnp.concatenate([w[:half], w[width : width + half]], axis=0)
    hi[...] = jnp.concatenate([w[half:width], w[width + half :]], axis=0)


def pair_product(left, right, dims):
    return lax.dot_general(left[0], right[0], dims, preferred_element_type=F32) + (
        lax.dot_general(left[0], right[1], dims, preferred_element_type=F32)
        + lax.dot_general(left[1], right[0], dims, preferred_element_type=F32)
    )


def a_kernel(index, fh, fl, ch, cl, out):
    factor = (fh[index].T, fl[index].T)
    out[...] = pair_product(factor, read((ch, cl)), NN)


def b_kernel(fh, fl, ch, cl, out):
    couple = (ch[...].T, cl[...].T)
    for index in range(2):
        out[index] = pair_product(couple, (fh[index], fl[index]), NT)


def roles_kernel(count, *refs):
    sources = (refs[:count], refs[count : 2 * count])
    high, low, buf, sems = refs[-4:]
    mine = lax.axis_index("row") % 2
    slots = (mine, 1 - mine)
    n = buf.shape[2]
    rows = n // (CHUNKS // 2)
    copies = []
    for side in range(2):
        halves = sources[side] if count == 2 else [sources[side][0].at[i] for i in range(2)]
        for index, half in enumerate(halves):
            for start in range(0, n, rows):
                part = pl.ds(start, rows)
                copy = pltpu.make_async_copy(
                    half.at[part], buf.at[side, index, part], sems.at[side, len(copies) % CHUNKS]
                )
                copy.start()
                copies.append((side, index, part, copy))
    for side, index, part, copy in copies:
        copy.wait()
        h, l = parts_of(buf[side, index, part, :])
        high[slots[side], index, part, :] = h
        low[slots[side], index, part, :] = l


def roles_and_vectors_kernel(count, *refs):
    v_own, v_other, va, vb = refs[2 * count : 2 * count + 4]
    roles_kernel(count, *refs[: 2 * count], *refs[-4:])
    mine = lax.axis_index("row") % 2
    half = va.shape[0]
    own = v_own[pl.ds(pl.multiple_of(mine * half, half), half), :]
    other = v_other[pl.ds(pl.multiple_of(mine * half, half), half), :]
    va[...] = jnp.where(mine == 0, own, other)
    vb[...] = jnp.where(mine == 0, other, own)


def roles(owns, others, vectors=()):
    n = others[0].shape[-1]
    shape = (2, 2, n, n)
    halves = [(v.shape[0] // 2, n) for v in vectors]
    body = roles_and_vectors_kernel if vectors else roles_kernel
    return pl.pallas_call(
        functools.partial(body, len(others)),
        out_shape=tuple(pltpu.VMEM(half, F32) for half in halves)
        + (pltpu.VMEM(shape, BF16), pltpu.VMEM(shape, BF16)),
        in_specs=[HBM] * (2 * len(others)) + [VMEM] * len(vectors),
        out_specs=(VMEM,) * (2 + len(halves)),
        scratch_shapes=[pltpu.VMEM(shape, F32), pltpu.SemaphoreType.DMA((2, CHUNKS))],
        compiler_params=pltpu.CompilerParams(vmem_limit_bytes=20 << 20),
    )(
        *[pltpu.with_memory_space_constraint(x, pltpu.HBM) for x in owns],
        *others,
        *[pltpu.with_memory_space_constraint(x, pltpu.VMEM) for x in vectors],
    )


def forward_kernel(*refs):
    *cs, va, vb, ah, al, out = refs
    c = cs[0][...]
    for other in cs[1:]:
        c = c + other[...]
    y = apply_to(add_real(c, va[...]), block_of((ah, al), 0), NN)
    out[...] = apply_to(add_real(y, vb[...]), block_of((ah, al), 1), NN)


def turn_kernel(c, va, vb, fh, fl, ah, al, bh, bl, ua, ub, s):
    y = add_real(c[...], va[...])
    y_b = add_real(apply_to(y, block_of((ah, al), 0), NN), vb[...])
    u_b = apply_to(y_b, block_of((fh, fl), 1), NT)
    u_a = apply_to(y, block_of((fh, fl), 0), NT)
    ub[...] = u_b
    ua[...] = u_a
    s[...] = u_a + apply_to(u_b, block_of((bh, bl), 0), NN)


def backward_kernel(r, ua, ub, bh, bl, xa, *xb):
    x_b = ub[...] + apply_to(r[...], block_of((bh, bl), 1), NN)
    for out in xb:
        out[...] = x_b
    xa[...] = ua[...] + apply_to(x_b, block_of((bh, bl), 0), NN)


def after(*values, every=False):
    held = lax.optimization_barrier(values)
    return held if every else held[0]


def tree_sum(values):
    while len(values) > 1:
        values = [values[i] + values[i + 1] for i in range(0, len(values), 2)]
    return values[0]


def shards(inv_factors, coupling, vectors):
    n = inv_factors.shape[3]
    width = vectors.shape[2]
    half = width // 2
    rows = lax.axis_size("row")
    nodes = lax.axis_size("node")
    layers = rows // 2
    core = lax.axis_index("row") % 2
    node = lax.axis_index("node")
    first = core == 0

    def swap_core(value):
        return lax.ppermute(value, "row", [(r, r ^ 1) for r in range(rows)])

    def hop(value, source, target):
        return lax.ppermute(value, "row", [(2 * source + c, 2 * target + c) for c in range(2)])

    def exchange_node(value, d):
        return lax.ppermute(value, "node", [(j, j ^ d) for j in range(nodes)])

    def exchange_layer(value, d):
        return lax.ppermute(value, "row", [(r, r ^ (2 * d)) for r in range(rows)])

    factor = inv_factors[0, 0]
    couple = coupling[0]
    block = ((2 * half, n), F32)

    fh, fl, ch, cl, v_t, g = pl.pallas_call(
        enter_kernel,
        out_shape=(
            pltpu.VMEM((2, n, n), BF16),
            pltpu.VMEM((2, n, n), BF16),
            pltpu.VMEM((n, n), BF16),
            pltpu.VMEM((n, n), BF16),
            pltpu.VMEM((width, n), F32),
            pltpu.VMEM((2 * width, n), F32),
        ),
        in_specs=[HBM] * 3,
        out_specs=(VMEM,) * 6,
        scratch_shapes=[
            pltpu.VMEM((2, n, n), F32),
            pltpu.VMEM((n, n), F32),
            pltpu.VMEM((width, n), F32),
            pltpu.SemaphoreType.DMA((CHUNKS + 2,)),
        ],
        compiler_params=pltpu.CompilerParams(vmem_limit_bytes=20 << 20),
        name="enter",
    )(*[pltpu.with_memory_space_constraint(x, pltpu.HBM) for x in (factor, couple, vectors[0].T)])
    from_a = swap_core(g)
    (a_re,) = call(functools.partial(a_kernel, 0), [((n, n), F32)], after(fh, g), fl, ch, cl)
    lo, hi = call(leave_kernel, [block, block], v_t, from_a, after(fh, from_a), fl, ch, cl)

    got_lo = lax.ppermute(lo, "row", [(1, 2)])
    got_hi = lax.ppermute(hi, "row", [(1, 3)])
    got = [got_lo, got_hi]
    (a_im,) = call(functools.partial(a_kernel, 1), [((n, n), F32)], after(fh, lo), fl, ch, cl)
    a_re_other = swap_core(after(a_re, from_a))
    a_im_other = swap_core(a_im)
    v_other = swap_core(after(v_t, lo))
    va, vb, *a_mats = roles([a_re, a_im], [a_re_other, a_im_other], [v_t, v_other])
    f_other = swap_core(after(factor, a_re_other, a_im_other))
    carry = jnp.zeros((2 * half, n), F32)
    for t in range(layers - 1):
        if t > 0:
            got = [hop(leaving, t, t + 1)]
        carry = sum(got, carry)
        if t < layers - 2:
            (leaving,) = call(forward_kernel, [block], *got, va, vb, *a_mats)
        if t == 0:
            f_mats = roles([after(factor, leaving)], [f_other])
            (b_own,) = call(b_kernel, [((2, n, n), F32)], after(fh, leaving), fl, ch, cl)
            b_other = swap_core(b_own)
        if t == 1:
            b_mats = roles([after(b_own, leaving)], [b_other])
    u_a, u_b, leaving = call(turn_kernel, [block] * 3, carry, va, vb, *f_mats, *a_mats, *b_mats)

    following = jnp.zeros((2 * half, n), F32)
    for t in range(layers - 1, 0, -1):
        got = hop(leaving, t, t - 1)
        following = following + got
        if t > 1:
            (leaving,) = call(backward_kernel, [block], got, u_a, u_b, *b_mats)
    x_a, x_b = call(backward_kernel, [block] * 2, following, u_a, u_b, *b_mats)

    share = n // nodes
    x_both = jnp.concatenate([x_a, x_b], axis=0)
    pieces = [lax.dynamic_slice_in_dim(x_both, (node ^ d) * share, share, 1) for d in range(nodes)]
    pieces = [pieces[0]] + [exchange_node(pieces[d], d) for d in range(1, nodes)]
    pieces = [p.reshape(2, 2, half, share) for p in pieces]
    terms = []
    for order in range(MOM):
        re_terms, im_terms = [], []
        for d in range(nodes):
            theta = 2.0 * math.pi * ((node ^ d).astype(F32) + 0.5) / nodes
            w_re = jnp.cos((order + 1) * theta) / nodes
            w_im = jnp.sin((order + 1) * theta) / nodes
            re, im = pieces[d][:, 0], pieces[d][:, 1]
            re_terms.append(w_re * re - w_im * im)
            im_terms.append(w_re * im + w_im * re)
        terms += [tree_sum(re_terms), tree_sum(im_terms)]
    mine = jnp.stack(terms, axis=1)
    groups = 2 * MOM
    cols = groups * width
    other = swap_core(mine.reshape(2 * groups * half, share)).reshape(mine.shape)
    both = jnp.stack([jnp.where(first, mine, other), jnp.where(first, other, mine)], axis=2)
    both = both.reshape(2, cols, share)
    moments = jnp.where(first, both[0], both[1])

    mine = mine.reshape(2, groups * half, share)
    gram = lax.dot_general(mine[0], both[0], NT, precision=PREC) + lax.dot_general(
        mine[1], both[1], NT, precision=PREC
    )
    hc = groups * half
    gs = hc // nodes
    own = [lax.dynamic_slice_in_dim(gram, (node ^ d) * gs, gs, 0) for d in range(nodes)]
    piece = tree_sum([own[0]] + [exchange_node(own[d], d) for d in range(1, nodes)])
    piece = tree_sum([piece] + [exchange_layer(piece, d) for d in range(1, layers)])
    piece = piece * (nodes / (rows * n))
    got = [piece] + [exchange_node(piece, d) for d in range(1, nodes)]
    gram = jnp.zeros((hc, cols), F32)
    for d in range(nodes):
        gram = lax.dynamic_update_slice_in_dim(gram, got[d], (node ^ d) * gs, 0)
    other = swap_core(gram)
    gram = gram.reshape(groups, half, cols)
    other = other.reshape(groups, half, cols)
    gram = jnp.stack([jnp.where(first, gram, other), jnp.where(first, other, gram)], axis=1)
    return moments.T[None], gram.reshape(cols, cols)


def solution(mesh):
    return jax.shard_map(
        shards,
        mesh=mesh,
        in_specs=(
            P(("intv", "node"), "row", None, None, None),
            P("row", None, None),
            P("row", None, None),
        ),
        out_specs=(P(("intv", "row"), "node", None), P("intv", None)),
        check_vma=False,
    )
```

```python
import functools
import functools
import math

import jax
import jax.numpy as jnp
from jax import lax
from jax.experimental import pallas as pl
from jax.experimental.pallas import tpu as pltpu
from jax.sharding import PartitionSpec as P


MOM = 2
F32, BF16 = jnp.float32, jnp.bfloat16
NN = (((1,), (0,)), ((), ()))
NT = (((1,), (1,)), ((), ()))
VMEM = pl.BlockSpec(memory_space=pltpu.VMEM)
HBM = pl.BlockSpec(memory_space=pltpu.HBM)
CHUNKS = 4
ENTER_CHUNKS = 2


def parts_of(x):
    high = x.astype(BF16)
    return high, (x - high.astype(F32)).astype(BF16)


def times(rows, matrix, dims):
    w = rows.shape[0]
    high, low = parts_of(rows)
    both = lax.dot_general(
        jnp.concatenate([high, low], axis=0), matrix[0], dims, preferred_element_type=F32
    )
    rest = lax.dot_general(high, matrix[1], dims, preferred_element_type=F32)
    return both[:w] + (both[w:] + rest)


def apply_to(rows, matrix, dims):
    w = rows.shape[0] // 2
    re, im = (times(rows, part, dims) for part in matrix)
    return jnp.concatenate([re[:w] - im[w:], im[:w] + re[w:]], axis=0)


def add_real(block, real):
    w = real.shape[0]
    return jnp.concatenate([block[:w] + real, block[w:]], axis=0)


def read(pair):
    return pair[0][...], pair[1][...]


def block_of(mats, role):
    return tuple((mats[0, role, part], mats[1, role, part]) for part in range(2))


def write(pair, value):
    high, low = parts_of(value)
    pair[0][...] = high
    pair[1][...] = low


def call(kernel, outs, *operands, scratch=()):
    return pl.pallas_call(
        kernel,
        out_shape=tuple(pltpu.VMEM(shape, dtype) for shape, dtype in outs),
        in_specs=[VMEM] * len(operands),
        out_specs=tuple([VMEM] * len(outs)),
        scratch_shapes=[pltpu.VMEM(shape, dtype) for shape, dtype in scratch],
        compiler_params=pltpu.CompilerParams(vmem_limit_bytes=20 << 20),
    )(*[pltpu.with_memory_space_constraint(x, pltpu.VMEM) for x in operands])


def enter_kernel(f_any, c_any, v_any, fh, fl, ch, cl, vt, g, f_buf, c_buf, v_buf, sems):
    n = c_buf.shape[0]
    per_part = ENTER_CHUNKS // 2
    rows = n // per_part
    v_copy = pltpu.make_async_copy(v_any, v_buf, sems.at[ENTER_CHUNKS])
    v_copy.start()
    copies = []
    places = [(i // per_part, pl.ds(i % per_part * rows, rows)) for i in range(ENTER_CHUNKS)]
    for i, place in enumerate(places):
        copies.append(pltpu.make_async_copy(f_any.at[place], f_buf.at[place], sems.at[i]))
        copies[-1].start()
    c_copy = pltpu.make_async_copy(c_any, c_buf, sems.at[ENTER_CHUNKS + 1])
    c_copy.start()
    v_copy.wait()
    real = v_buf[...]
    vt[...] = real
    pieces = []
    for copy, place in zip(copies, places):
        copy.wait()
        high, low = parts_of(f_buf[place])
        fh[place] = high
        fl[place] = low
        pieces.append(times(real, (high, low), NT))
    q = jnp.concatenate(pieces, axis=1)
    u = jnp.concatenate([q[:, :n], q[:, n:]], axis=0)
    c_copy.wait()
    write((ch, cl), c_buf[...])
    g[...] = times(u, read((ch, cl)), NN)


def leave_kernel(vt, g, fh, fl, ch, cl, lo, hi):
    y = add_real(g[...], vt[...])
    w = times(apply_to(y, tuple((fh[part], fl[part]) for part in range(2)), NT), read((ch, cl)), NN)
    half = lo.shape[0] // 2
    width = 2 * half
    lo[...] = jnp.concatenate([w[:half], w[width : width + half]], axis=0)
    hi[...] = jnp.concatenate([w[half:width], w[width + half :]], axis=0)


def pair_product(left, right, dims):
    return lax.dot_general(left[0], right[0], dims, preferred_element_type=F32) + (
        lax.dot_general(left[0], right[1], dims, preferred_element_type=F32)
        + lax.dot_general(left[1], right[0], dims, preferred_element_type=F32)
    )


def a_kernel(index, fh, fl, ch, cl, out):
    factor = (fh[index].T, fl[index].T)
    out[...] = pair_product(factor, read((ch, cl)), NN)


def b_kernel(fh, fl, ch, cl, out):
    couple = (ch[...].T, cl[...].T)
    for index in range(2):
        out[index] = pair_product(couple, (fh[index], fl[index]), NT)


def roles_kernel(count, *refs):
    sources = (refs[:count], refs[count : 2 * count])
    mats, buf, sems = refs[-3:]
    mine = lax.axis_index("row") % 2
    slots = (mine, 1 - mine)
    n = buf.shape[2]
    rows = n // (CHUNKS // 2)
    copies = []
    for side in range(2):
        halves = sources[side] if count == 2 else [sources[side][0].at[i] for i in range(2)]
        for index, half in enumerate(halves):
            for start in range(0, n, rows):
                part = pl.ds(start, rows)
                copy = pltpu.make_async_copy(
                    half.at[part], buf.at[side, index, part], sems.at[side, len(copies) % CHUNKS]
                )
                copy.start()
                copies.append((side, index, part, copy))
    for side, index, part, copy in copies:
        copy.wait()
        h, l = parts_of(buf[side, index, part, :])
        mats[0, slots[side], index, part, :] = h
        mats[1, slots[side], index, part, :] = l


def roles_and_vectors_kernel(count, *refs):
    v_own, v_other, va, vb = refs[2 * count : 2 * count + 4]
    roles_kernel(count, *refs[: 2 * count], *refs[-3:])
    mine = lax.axis_index("row") % 2
    half = va.shape[0]
    own = v_own[pl.ds(pl.multiple_of(mine * half, half), half), :]
    other = v_other[pl.ds(pl.multiple_of(mine * half, half), half), :]
    va[...] = jnp.where(mine == 0, own, other)
    vb[...] = jnp.where(mine == 0, other, own)


def roles(owns, others, vectors=()):
    n = others[0].shape[-1]
    shape = (2, 2, 2, n, n)
    halves = [(v.shape[0] // 2, n) for v in vectors]
    body = roles_and_vectors_kernel if vectors else roles_kernel
    return pl.pallas_call(
        functools.partial(body, len(others)),
        out_shape=tuple(pltpu.VMEM(half, F32) for half in halves)
        + (pltpu.VMEM(shape, BF16),),
        in_specs=[HBM] * (2 * len(others)) + [VMEM] * len(vectors),
        out_specs=(VMEM,) * (1 + len(halves)),
        scratch_shapes=[pltpu.VMEM(shape[1:], F32), pltpu.SemaphoreType.DMA((2, CHUNKS))],
        compiler_params=pltpu.CompilerParams(vmem_limit_bytes=20 << 20),
    )(
        *[pltpu.with_memory_space_constraint(x, pltpu.HBM) for x in owns],
        *others,
        *[pltpu.with_memory_space_constraint(x, pltpu.VMEM) for x in vectors],
    )


def total(refs):
    value = refs[0][...]
    for other in refs[1:]:
        value = value + other[...]
    return value


def forward_kernel(*refs):
    *cs, va, vb, a_mats, out = refs
    y = apply_to(add_real(total(cs), va[...]), block_of(a_mats, 0), NN)
    out[...] = apply_to(add_real(y, vb[...]), block_of(a_mats, 1), NN)


def turn_kernel(*refs):
    *cs, va, vb, f_mats, a_mats, b_mats, ua, ub, s, weights = refs
    nodes = lax.axis_size("node")
    line = lax.broadcasted_iota(jnp.int32, weights.shape, 0)
    other, kind = line % nodes, line // nodes
    theta = 2.0 * math.pi * ((lax.axis_index("node") ^ other).astype(F32) + 0.5) / nodes
    angle = (kind // 2 + 1).astype(F32) * theta
    weights[...] = jnp.where(kind % 2 == 0, jnp.cos(angle), jnp.sin(angle)) / nodes
    y = add_real(total(cs), va[...])
    y_b = add_real(apply_to(y, block_of(a_mats, 0), NN), vb[...])
    u_b = apply_to(y_b, block_of(f_mats, 1), NT)
    u_a = apply_to(y, block_of(f_mats, 0), NT)
    ub[...] = u_b
    ua[...] = u_a
    s[...] = u_a + apply_to(u_b, block_of(b_mats, 0), NN)


def backward_kernel(r, ua, ub, b_mats, xa):
    x_b = ub[...] + apply_to(r[...], block_of(b_mats, 1), NN)
    xa[...] = ua[...] + apply_to(x_b, block_of(b_mats, 0), NN)


def leave_backward_kernel(shares, *refs):
    *rs, ua, ub, b_mats = refs[: -1 - shares]
    *pieces, x = refs[-1 - shares :]
    node = lax.axis_index("node")
    x_b = ub[...] + apply_to(total(rs), block_of(b_mats, 1), NN)
    rows = x_b.shape[0]
    x[pl.ds(rows, rows), :] = x_b
    x[pl.ds(0, rows), :] = ua[...] + apply_to(x_b, block_of(b_mats, 0), NN)
    for d, piece in enumerate(pieces):
        lanes = piece.shape[1]
        piece[...] = x[:, pl.ds(pl.multiple_of((node ^ d) * lanes, lanes), lanes)]


def combine_kernel(*refs):
    *pieces, weights, out = refs
    nodes = len(pieces)
    half = pieces[0].shape[0] // 4
    share = out.shape[1]
    groups = 2 * MOM
    for b in range(2):
        parts = [
            [piece[pl.ds((2 * b + part) * half, half), :] for piece in pieces] for part in range(2)
        ]
        for order in range(MOM):
            w_re, w_im = (
                [weights[pl.ds((2 * order + part) * nodes + d, 1), :][:, :share] for d in range(nodes)]
                for part in range(2)
            )
            re = [w_re[d] * parts[0][d] - w_im[d] * parts[1][d] for d in range(nodes)]
            im = [w_re[d] * parts[1][d] + w_im[d] * parts[0][d] for d in range(nodes)]
            row = (b * groups + 2 * order) * half
            out[pl.ds(row, half), :] = tree_sum(re)
            out[pl.ds(row + half, half), :] = tree_sum(im)


def gram_kernel(mine, other, moments, *outs):
    *owns, buf = outs
    node = lax.axis_index("node")
    first = lax.axis_index("row") % 2 == 0
    groups = 2 * MOM
    half = mine.shape[0] // (2 * groups)
    gram, both = None, []
    for b in range(2):
        part = pl.ds(b * groups * half, groups * half)
        a, o = mine[part, :], other[part, :]
        lo, hi = jnp.where(first, a, o), jnp.where(first, o, a)
        cuts = [slice(g * half, (g + 1) * half) for g in range(groups)]
        both.append(jnp.concatenate([side[cut] for cut in cuts for side in (lo, hi)], axis=0))
        product = times(a, parts_of(both[b]), NT)
        gram = product if gram is None else gram + product
    buf[...] = gram
    for d, own in enumerate(owns):
        rows = own.shape[0]
        own[...] = buf[pl.ds(pl.multiple_of((node ^ d) * rows, rows), rows), :]
    moments[...] = jnp.where(first, both[0], both[1])


def gather_kernel(*refs):
    *pieces, out = refs
    node = lax.axis_index("node")
    for d, piece in enumerate(pieces):
        rows = piece.shape[0]
        out[pl.ds(pl.multiple_of((node ^ d) * rows, rows), rows), :] = piece[...]


def join_kernel(mine, other, out):
    first = lax.axis_index("row") % 2 == 0
    groups = 2 * MOM
    half = mine.shape[0] // groups
    for g in range(groups):
        cut = pl.ds(g * half, half)
        out[pl.ds(2 * g * half, half), :] = jnp.where(first, mine[cut, :], other[cut, :])
        out[pl.ds((2 * g + 1) * half, half), :] = jnp.where(first, other[cut, :], mine[cut, :])


def after(*values, every=False):
    held = lax.optimization_barrier(values)
    return held if every else held[0]


def tree_sum(values):
    while len(values) > 1:
        values = [values[i] + values[i + 1] for i in range(0, len(values), 2)]
    return values[0]


def shards(inv_factors, coupling, vectors):
    n = inv_factors.shape[3]
    width = vectors.shape[2]
    half = width // 2
    rows = lax.axis_size("row")
    nodes = lax.axis_size("node")
    layers = rows // 2

    def swap_core(value):
        return lax.ppermute(value, "row", [(r, r ^ 1) for r in range(rows)])

    def hop(value, source, target):
        return lax.ppermute(value, "row", [(2 * source + c, 2 * target + c) for c in range(2)])

    def exchange_node(value, d):
        return lax.ppermute(value, "node", [(j, j ^ d) for j in range(nodes)])

    def exchange_layer(value, d):
        return lax.ppermute(value, "row", [(r, r ^ (2 * d)) for r in range(rows)])

    factor = inv_factors[0, 0]
    couple = coupling[0]
    block = ((2 * half, n), F32)

    fh, fl, ch, cl, v_t, g = pl.pallas_call(
        enter_kernel,
        out_shape=(
            pltpu.VMEM((2, n, n), BF16),
            pltpu.VMEM((2, n, n), BF16),
            pltpu.VMEM((n, n), BF16),
            pltpu.VMEM((n, n), BF16),
            pltpu.VMEM((width, n), F32),
            pltpu.VMEM((2 * width, n), F32),
        ),
        in_specs=[HBM] * 3,
        out_specs=(VMEM,) * 6,
        scratch_shapes=[
            pltpu.VMEM((2, n, n), F32),
            pltpu.VMEM((n, n), F32),
            pltpu.VMEM((width, n), F32),
            pltpu.SemaphoreType.DMA((ENTER_CHUNKS + 2,)),
        ],
        compiler_params=pltpu.CompilerParams(vmem_limit_bytes=20 << 20),
        name="enter",
    )(*[pltpu.with_memory_space_constraint(x, pltpu.HBM) for x in (factor, couple, vectors[0].T)])
    from_a = swap_core(g)
    (a_re,) = call(functools.partial(a_kernel, 0), [((n, n), F32)], after(fh, g), fl, ch, cl)
    lo, hi = call(leave_kernel, [block, block], v_t, from_a, after(fh, from_a), fl, ch, cl)

    got_lo = lax.ppermute(lo, "row", [(1, 2)])
    got_hi = lax.ppermute(hi, "row", [(1, 3)])
    got = [got_lo, got_hi]
    (a_im,) = call(functools.partial(a_kernel, 1), [((n, n), F32)], after(fh, lo), fl, ch, cl)
    a_re_other = swap_core(after(a_re, from_a))
    a_im_other = swap_core(a_im)
    v_other = swap_core(after(v_t, lo))
    va, vb, a_mats = roles([a_re, a_im], [a_re_other, a_im_other], [v_t, v_other])
    f_other = swap_core(after(factor, a_re_other, a_im_other))
    arrived = []
    for t in range(layers - 1):
        if t > 0:
            got = [hop(leaving, t, t + 1)]
        arrived += got
        if t < layers - 2:
            (leaving,) = call(forward_kernel, [block], *got, va, vb, a_mats)
        if t == 0:
            (f_mats,) = roles([after(factor, leaving)], [f_other])
            (b_own,) = call(b_kernel, [((2, n, n), F32)], after(fh, leaving), fl, ch, cl)
            b_other = swap_core(b_own)
        if t == 1:
            (b_mats,) = roles([after(b_own, leaving, f_mats)], [b_other])
    u_a, u_b, leaving, weights = call(
        turn_kernel, [block] * 3 + [((2 * MOM * nodes, 128), F32)], *arrived, va, vb, f_mats, a_mats, b_mats
    )

    arrived = []
    for t in range(layers - 1, 0, -1):
        got = hop(leaving, t, t - 1)
        arrived.append(got)
        if t > 1:
            (leaving,) = call(backward_kernel, [block], got, u_a, u_b, b_mats)
    share = n // nodes
    shares = nodes if share % 128 == 0 else 0
    x_both = ((4 * half, n), F32)
    pieces = call(
        functools.partial(leave_backward_kernel, shares),
        [((4 * half, share), F32)] * shares or [x_both],
        *arrived, u_a, u_b, b_mats,
        scratch=[x_both] if shares else [],
    )

    if not shares:
        node = lax.axis_index("node")
        pieces = [
            lax.dynamic_slice_in_dim(pieces[0], (node ^ d) * share, share, 1)
            for d in range(nodes)
        ]
    pieces = [pieces[0]] + [exchange_node(pieces[d], d) for d in range(1, nodes)]
    groups = 2 * MOM
    cols = groups * width
    (mine,) = call(combine_kernel, [((2 * groups * half, share), F32)], *pieces, weights)
    other = swap_core(mine)

    hc = groups * half
    gs = hc // nodes
    moments, *own = call(
        gram_kernel,
        [((cols, share), F32)] + [((gs, cols), F32)] * nodes,
        mine, other,
        scratch=[((hc, cols), F32)],
    )
    piece = tree_sum([own[0]] + [exchange_node(own[d], d) for d in range(1, nodes)])
    piece = tree_sum([piece] + [exchange_layer(piece, d) for d in range(1, layers)])
    piece = piece * (nodes / (rows * n))
    got = [piece] + [exchange_node(piece, d) for d in range(1, nodes)]
    (gram,) = call(gather_kernel, [((hc, cols), F32)], *got)
    other = swap_core(gram)
    gram = pl.pallas_call(
        join_kernel,
        out_shape=jax.ShapeDtypeStruct((cols, cols), F32),
        in_specs=[VMEM] * 2,
        out_specs=VMEM,
        compiler_params=pltpu.CompilerParams(vmem_limit_bytes=20 << 20),
        name="join",
    )(*[pltpu.with_memory_space_constraint(x, pltpu.VMEM) for x in (gram, other)])
    return moments.T[None], gram


def solution(mesh):
    return jax.shard_map(
        shards,
        mesh=mesh,
        in_specs=(
            P(("intv", "node"), "row", None, None, None),
            P("row", None, None),
            P("row", None, None),
        ),
        out_specs=(P(("intv", "row"), "node", None), P("intv", None)),
        check_vma=False,
    )
```

```python
import functools
import functools
import math

import jax
import jax.numpy as jnp
from jax import lax
from jax.experimental import pallas as pl
from jax.experimental.pallas import tpu as pltpu
from jax.sharding import PartitionSpec as P


MOM = 2
F32, BF16 = jnp.float32, jnp.bfloat16
NN = (((1,), (0,)), ((), ()))
NT = (((1,), (1,)), ((), ()))
VMEM = pl.BlockSpec(memory_space=pltpu.VMEM)
HBM = pl.BlockSpec(memory_space=pltpu.HBM)
CHUNKS = 4
ENTER_CHUNKS = 2


def parts_of(x):
    high = x.astype(BF16)
    return high, (x - high.astype(F32)).astype(BF16)


def times(rows, matrix, dims):
    w = rows.shape[0]
    high, low = parts_of(rows)
    both = lax.dot_general(
        jnp.concatenate([high, low], axis=0), matrix[0], dims, preferred_element_type=F32
    )
    rest = lax.dot_general(high, matrix[1], dims, preferred_element_type=F32)
    return both[:w] + (both[w:] + rest)


def apply_to(rows, matrix, dims):
    w = rows.shape[0] // 2
    re, im = (times(rows, part, dims) for part in matrix)
    return jnp.concatenate([re[:w] - im[w:], im[:w] + re[w:]], axis=0)


def add_real(block, real):
    w = real.shape[0]
    return jnp.concatenate([block[:w] + real, block[w:]], axis=0)


def read(pair):
    return pair[0][...], pair[1][...]


def block_of(mats, role):
    return tuple((mats[0, role, part], mats[1, role, part]) for part in range(2))


def write(pair, value):
    high, low = parts_of(value)
    pair[0][...] = high
    pair[1][...] = low


def call(kernel, outs, *operands, scratch=()):
    return pl.pallas_call(
        kernel,
        out_shape=tuple(pltpu.VMEM(shape, dtype) for shape, dtype in outs),
        in_specs=[VMEM] * len(operands),
        out_specs=tuple([VMEM] * len(outs)),
        scratch_shapes=[pltpu.VMEM(shape, dtype) for shape, dtype in scratch],
        compiler_params=pltpu.CompilerParams(vmem_limit_bytes=20 << 20),
    )(*[pltpu.with_memory_space_constraint(x, pltpu.VMEM) for x in operands])


def enter_kernel(f_any, c_any, v_any, fh, fl, ch, cl, vt, g, f_buf, c_buf, v_buf, sems):
    n = c_buf.shape[0]
    per_part = ENTER_CHUNKS // 2
    rows = n // per_part
    v_copy = pltpu.make_async_copy(v_any, v_buf, sems.at[ENTER_CHUNKS])
    v_copy.start()
    copies = []
    places = [(i // per_part, pl.ds(i % per_part * rows, rows)) for i in range(ENTER_CHUNKS)]
    for i, place in enumerate(places):
        copies.append(pltpu.make_async_copy(f_any.at[place], f_buf.at[place], sems.at[i]))
        copies[-1].start()
    c_copy = pltpu.make_async_copy(c_any, c_buf, sems.at[ENTER_CHUNKS + 1])
    c_copy.start()
    v_copy.wait()
    real = v_buf[...]
    vt[...] = real
    pieces = []
    for copy, place in zip(copies, places):
        copy.wait()
        high, low = parts_of(f_buf[place])
        fh[place] = high
        fl[place] = low
        pieces.append(times(real, (high, low), NT))
    q = jnp.concatenate(pieces, axis=1)
    u = jnp.concatenate([q[:, :n], q[:, n:]], axis=0)
    c_copy.wait()
    write((ch, cl), c_buf[...])
    g[...] = times(u, read((ch, cl)), NN)


def leave_kernel(vt, g, fh, fl, ch, cl, lo, hi):
    y = add_real(g[...], vt[...])
    w = times(apply_to(y, tuple((fh[part], fl[part]) for part in range(2)), NT), read((ch, cl)), NN)
    half = lo.shape[0] // 2
    width = 2 * half
    lo[...] = jnp.concatenate([w[:half], w[width : width + half]], axis=0)
    hi[...] = jnp.concatenate([w[half:width], w[width + half :]], axis=0)


def pair_product(left, right, dims):
    return lax.dot_general(left[0], right[0], dims, preferred_element_type=F32) + (
        lax.dot_general(left[0], right[1], dims, preferred_element_type=F32)
        + lax.dot_general(left[1], right[0], dims, preferred_element_type=F32)
    )


def a_kernel(index, fh, fl, ch, cl, out):
    factor = (fh[index].T, fl[index].T)
    out[...] = pair_product(factor, read((ch, cl)), NN)


def b_kernel(fh, fl, ch, cl, out):
    couple = (ch[...].T, cl[...].T)
    for index in range(2):
        out[index] = pair_product(couple, (fh[index], fl[index]), NT)


def roles_kernel(count, *refs):
    sources = (refs[:count], refs[count : 2 * count])
    mats, buf, sems = refs[-3:]
    mine = lax.axis_index("row") % 2
    slots = (mine, 1 - mine)
    n = buf.shape[2]
    rows = n // (CHUNKS // 2)
    copies = []
    for side in range(2):
        halves = sources[side] if count == 2 else [sources[side][0].at[i] for i in range(2)]
        for index, half in enumerate(halves):
            for start in range(0, n, rows):
                part = pl.ds(start, rows)
                copy = pltpu.make_async_copy(
                    half.at[part], buf.at[side, index, part], sems.at[side, len(copies) % CHUNKS]
                )
                copy.start()
                copies.append((side, index, part, copy))
    for side, index, part, copy in copies:
        copy.wait()
        h, l = parts_of(buf[side, index, part, :])
        mats[0, slots[side], index, part, :] = h
        mats[1, slots[side], index, part, :] = l


def resident_roles_kernel(count, *refs):
    sources, mats = (refs[:count], refs[count : 2 * count]), refs[-1]
    mine = lax.axis_index("row") % 2
    for side, slot in enumerate((mine, 1 - mine)):
        for index in range(2):
            value = sources[side][index][...] if count == 2 else sources[side][0][index]
            mats[0, slot, index], mats[1, slot, index] = parts_of(value)


def roles_and_vectors_kernel(count, *refs):
    v_own, v_other, va, vb, mats = refs[2 * count :]
    resident_roles_kernel(count, *refs[: 2 * count], mats)
    mine = lax.axis_index("row") % 2
    half = va.shape[0]
    own = v_own[pl.ds(pl.multiple_of(mine * half, half), half), :]
    other = v_other[pl.ds(pl.multiple_of(mine * half, half), half), :]
    va[...] = jnp.where(mine == 0, own, other)
    vb[...] = jnp.where(mine == 0, other, own)


def resident_roles(owns, others, vectors=()):
    n = others[0].shape[-1]
    halves = [((v.shape[0] // 2, n), F32) for v in vectors]
    body = roles_and_vectors_kernel if vectors else resident_roles_kernel
    return call(
        functools.partial(body, len(others)),
        halves + [((2, 2, 2, n, n), BF16)],
        *owns, *others, *vectors,
    )


def roles(owns, others):
    n = others[0].shape[-1]
    shape = (2, 2, 2, n, n)
    return pl.pallas_call(
        functools.partial(roles_kernel, len(others)),
        out_shape=(pltpu.VMEM(shape, BF16),),
        in_specs=[HBM] * (2 * len(others)),
        out_specs=(VMEM,),
        scratch_shapes=[pltpu.VMEM(shape[1:], F32), pltpu.SemaphoreType.DMA((2, CHUNKS))],
        compiler_params=pltpu.CompilerParams(vmem_limit_bytes=20 << 20),
    )(*[pltpu.with_memory_space_constraint(x, pltpu.HBM) for x in owns], *others)


def total(refs):
    value = refs[0][...]
    for other in refs[1:]:
        value = value + other[...]
    return value


def forward_kernel(*refs):
    *cs, va, vb, a_mats, out = refs
    y = apply_to(add_real(total(cs), va[...]), block_of(a_mats, 0), NN)
    out[...] = apply_to(add_real(y, vb[...]), block_of(a_mats, 1), NN)


def turn_kernel(*refs):
    *cs, va, vb, f_mats, a_mats, b_mats, ua, ub, s, weights = refs
    nodes = lax.axis_size("node")
    line = lax.broadcasted_iota(jnp.int32, weights.shape, 0)
    other, kind = line % nodes, line // nodes
    theta = 2.0 * math.pi * ((lax.axis_index("node") ^ other).astype(F32) + 0.5) / nodes
    angle = (kind // 2 + 1).astype(F32) * theta
    weights[...] = jnp.where(kind % 2 == 0, jnp.cos(angle), jnp.sin(angle)) / nodes
    y = add_real(total(cs), va[...])
    y_b = add_real(apply_to(y, block_of(a_mats, 0), NN), vb[...])
    u_b = apply_to(y_b, block_of(f_mats, 1), NT)
    u_a = apply_to(y, block_of(f_mats, 0), NT)
    ub[...] = u_b
    ua[...] = u_a
    s[...] = u_a + apply_to(u_b, block_of(b_mats, 0), NN)


def backward_kernel(r, ua, ub, b_mats, xa):
    x_b = ub[...] + apply_to(r[...], block_of(b_mats, 1), NN)
    xa[...] = ua[...] + apply_to(x_b, block_of(b_mats, 0), NN)


def leave_backward_kernel(shares, *refs):
    *rs, ua, ub, b_mats = refs[: -1 - shares]
    *pieces, x = refs[-1 - shares :]
    node = lax.axis_index("node")
    x_b = ub[...] + apply_to(total(rs), block_of(b_mats, 1), NN)
    rows = x_b.shape[0]
    x[pl.ds(rows, rows), :] = x_b
    x[pl.ds(0, rows), :] = ua[...] + apply_to(x_b, block_of(b_mats, 0), NN)
    for d, piece in enumerate(pieces):
        lanes = piece.shape[1]
        piece[...] = x[:, pl.ds(pl.multiple_of((node ^ d) * lanes, lanes), lanes)]


def combine_kernel(*refs):
    *pieces, weights, out = refs
    nodes = len(pieces)
    half = pieces[0].shape[0] // 4
    share = out.shape[1]
    groups = 2 * MOM
    for b in range(2):
        parts = [
            [piece[pl.ds((2 * b + part) * half, half), :] for piece in pieces] for part in range(2)
        ]
        for order in range(MOM):
            w_re, w_im = (
                [weights[pl.ds((2 * order + part) * nodes + d, 1), :][:, :share] for d in range(nodes)]
                for part in range(2)
            )
            re = [w_re[d] * parts[0][d] - w_im[d] * parts[1][d] for d in range(nodes)]
            im = [w_re[d] * parts[1][d] + w_im[d] * parts[0][d] for d in range(nodes)]
            row = (b * groups + 2 * order) * half
            out[pl.ds(row, half), :] = tree_sum(re)
            out[pl.ds(row + half, half), :] = tree_sum(im)


def gram_kernel(mine, other, moments, *outs):
    *owns, buf = outs
    node = lax.axis_index("node")
    first = lax.axis_index("row") % 2 == 0
    groups = 2 * MOM
    half = mine.shape[0] // (2 * groups)
    gram, both = None, []
    for b in range(2):
        part = pl.ds(b * groups * half, groups * half)
        a, o = mine[part, :], other[part, :]
        lo, hi = jnp.where(first, a, o), jnp.where(first, o, a)
        cuts = [slice(g * half, (g + 1) * half) for g in range(groups)]
        both.append(jnp.concatenate([side[cut] for cut in cuts for side in (lo, hi)], axis=0))
        product = times(a, parts_of(both[b]), NT)
        gram = product if gram is None else gram + product
    buf[...] = gram
    for d, own in enumerate(owns):
        rows = own.shape[0]
        own[...] = buf[pl.ds(pl.multiple_of((node ^ d) * rows, rows), rows), :]
    moments[...] = jnp.where(first, both[0], both[1])


def gather_kernel(*refs):
    *pieces, out = refs
    node = lax.axis_index("node")
    for d, piece in enumerate(pieces):
        rows = piece.shape[0]
        out[pl.ds(pl.multiple_of((node ^ d) * rows, rows), rows), :] = piece[...]


def join_kernel(mine, other, out):
    first = lax.axis_index("row") % 2 == 0
    groups = 2 * MOM
    half = mine.shape[0] // groups
    for g in range(groups):
        cut = pl.ds(g * half, half)
        out[pl.ds(2 * g * half, half), :] = jnp.where(first, mine[cut, :], other[cut, :])
        out[pl.ds((2 * g + 1) * half, half), :] = jnp.where(first, other[cut, :], mine[cut, :])


def after(*values, every=False):
    held = lax.optimization_barrier(values)
    return held if every else held[0]


def tree_sum(values):
    while len(values) > 1:
        values = [values[i] + values[i + 1] for i in range(0, len(values), 2)]
    return values[0]


def shards(inv_factors, coupling, vectors):
    n = inv_factors.shape[3]
    width = vectors.shape[2]
    half = width // 2
    rows = lax.axis_size("row")
    nodes = lax.axis_size("node")
    layers = rows // 2

    def swap_core(value):
        return lax.ppermute(value, "row", [(r, r ^ 1) for r in range(rows)])

    def hop(value, source, target):
        return lax.ppermute(value, "row", [(2 * source + c, 2 * target + c) for c in range(2)])

    def exchange_node(value, d):
        return lax.ppermute(value, "node", [(j, j ^ d) for j in range(nodes)])

    def exchange_layer(value, d):
        return lax.ppermute(value, "row", [(r, r ^ (2 * d)) for r in range(rows)])

    factor = inv_factors[0, 0]
    couple = coupling[0]
    block = ((2 * half, n), F32)

    fh, fl, ch, cl, v_t, g = pl.pallas_call(
        enter_kernel,
        out_shape=(
            pltpu.VMEM((2, n, n), BF16),
            pltpu.VMEM((2, n, n), BF16),
            pltpu.VMEM((n, n), BF16),
            pltpu.VMEM((n, n), BF16),
            pltpu.VMEM((width, n), F32),
            pltpu.VMEM((2 * width, n), F32),
        ),
        in_specs=[HBM] * 3,
        out_specs=(VMEM,) * 6,
        scratch_shapes=[
            pltpu.VMEM((2, n, n), F32),
            pltpu.VMEM((n, n), F32),
            pltpu.VMEM((width, n), F32),
            pltpu.SemaphoreType.DMA((ENTER_CHUNKS + 2,)),
        ],
        compiler_params=pltpu.CompilerParams(vmem_limit_bytes=20 << 20),
        name="enter",
    )(*[pltpu.with_memory_space_constraint(x, pltpu.HBM) for x in (factor, couple, vectors[0].T)])
    from_a = swap_core(g)
    (a_re,) = call(functools.partial(a_kernel, 0), [((n, n), F32)], after(fh, g), fl, ch, cl)
    lo, hi = call(leave_kernel, [block, block], v_t, from_a, after(fh, from_a), fl, ch, cl)

    got_lo = lax.ppermute(lo, "row", [(1, 2)])
    got_hi = lax.ppermute(hi, "row", [(1, 3)])
    got = [got_lo, got_hi]
    (a_im,) = call(functools.partial(a_kernel, 1), [((n, n), F32)], after(fh, lo), fl, ch, cl)
    a_re_other = swap_core(after(a_re, from_a))
    a_im_other = swap_core(a_im)
    v_other = swap_core(after(v_t, lo))
    va, vb, a_mats = resident_roles([a_re, a_im], [a_re_other, a_im_other], [v_t, v_other])
    f_other = swap_core(after(factor, a_re_other, a_im_other))
    arrived = []
    for t in range(layers - 1):
        if t > 0:
            got = [hop(leaving, t, t + 1)]
        arrived += got
        if t < layers - 2:
            (leaving,) = call(forward_kernel, [block], *got, va, vb, a_mats)
        if t == 0:
            (f_mats,) = roles([after(factor, leaving)], [f_other])
            (b_own,) = call(b_kernel, [((2, n, n), F32)], after(fh, leaving), fl, ch, cl)
            b_other = swap_core(b_own)
        if t == 1:
            (b_mats,) = resident_roles([after(b_own, leaving, f_mats)], [b_other])
    u_a, u_b, leaving, weights = call(
        turn_kernel, [block] * 3 + [((2 * MOM * nodes, 128), F32)], *arrived, va, vb, f_mats, a_mats, b_mats
    )

    arrived = []
    for t in range(layers - 1, 0, -1):
        got = hop(leaving, t, t - 1)
        arrived.append(got)
        if t > 1:
            (leaving,) = call(backward_kernel, [block], got, u_a, u_b, b_mats)
    share = n // nodes
    shares = nodes if share % 128 == 0 else 0
    x_both = ((4 * half, n), F32)
    pieces = call(
        functools.partial(leave_backward_kernel, shares),
        [((4 * half, share), F32)] * shares or [x_both],
        *arrived, u_a, u_b, b_mats,
        scratch=[x_both] if shares else [],
    )

    if not shares:
        node = lax.axis_index("node")
        pieces = [
            lax.dynamic_slice_in_dim(pieces[0], (node ^ d) * share, share, 1)
            for d in range(nodes)
        ]
    pieces = [pieces[0]] + [exchange_node(pieces[d], d) for d in range(1, nodes)]
    groups = 2 * MOM
    cols = groups * width
    (mine,) = call(combine_kernel, [((2 * groups * half, share), F32)], *pieces, weights)
    other = swap_core(mine)

    hc = groups * half
    gs = hc // nodes
    moments, *own = call(
        gram_kernel,
        [((cols, share), F32)] + [((gs, cols), F32)] * nodes,
        mine, other,
        scratch=[((hc, cols), F32)],
    )
    piece = tree_sum([own[0]] + [exchange_node(own[d], d) for d in range(1, nodes)])
    piece = tree_sum([piece] + [exchange_layer(piece, d) for d in range(1, layers)])
    piece = piece * (nodes / (rows * n))
    got = [piece] + [exchange_node(piece, d) for d in range(1, nodes)]
    (gram,) = call(gather_kernel, [((hc, cols), F32)], *got)
    other = swap_core(gram)
    gram = pl.pallas_call(
        join_kernel,
        out_shape=jax.ShapeDtypeStruct((cols, cols), F32),
        in_specs=[VMEM] * 2,
        out_specs=VMEM,
        compiler_params=pltpu.CompilerParams(vmem_limit_bytes=20 << 20),
        name="join",
    )(*[pltpu.with_memory_space_constraint(x, pltpu.VMEM) for x in (gram, other)])
    return moments.T[None], gram


def solution(mesh):
    return jax.shard_map(
        shards,
        mesh=mesh,
        in_specs=(
            P(("intv", "node"), "row", None, None, None),
            P("row", None, None),
            P("row", None, None),
        ),
        out_specs=(P(("intv", "row"), "node", None), P("intv", None)),
        check_vma=False,
    )
```

```python
import functools
import functools
import math

import jax
import jax.numpy as jnp
from jax import lax
from jax.experimental import pallas as pl
from jax.experimental.pallas import tpu as pltpu
from jax.sharding import PartitionSpec as P


MOM = 2
F32, BF16 = jnp.float32, jnp.bfloat16
NN = (((1,), (0,)), ((), ()))
NT = (((1,), (1,)), ((), ()))
VMEM = pl.BlockSpec(memory_space=pltpu.VMEM)
HBM = pl.BlockSpec(memory_space=pltpu.HBM)
CHUNKS = 4
ENTER_CHUNKS = 2


def parts_of(x):
    high = x.astype(BF16)
    return high, (x - high.astype(F32)).astype(BF16)


def times(rows, matrix, dims):
    w = rows.shape[0]
    high, low = parts_of(rows)
    both = lax.dot_general(
        jnp.concatenate([high, low], axis=0), matrix[0], dims, preferred_element_type=F32
    )
    rest = lax.dot_general(high, matrix[1], dims, preferred_element_type=F32)
    return both[:w] + (both[w:] + rest)


def apply_to(rows, matrix, dims):
    w = rows.shape[0] // 2
    re, im = (times(rows, part, dims) for part in matrix)
    return jnp.concatenate([re[:w] - im[w:], im[:w] + re[w:]], axis=0)


def add_real(block, real):
    w = real.shape[0]
    return jnp.concatenate([block[:w] + real, block[w:]], axis=0)


def read(pair):
    return pair[0][...], pair[1][...]


def block_of(mats, role):
    return tuple((mats[0, role, part], mats[1, role, part]) for part in range(2))


def write(pair, value):
    high, low = parts_of(value)
    pair[0][...] = high
    pair[1][...] = low


def call(kernel, outs, *operands, scratch=()):
    return pl.pallas_call(
        kernel,
        out_shape=tuple(pltpu.VMEM(shape, dtype) for shape, dtype in outs),
        in_specs=[VMEM] * len(operands),
        out_specs=tuple([VMEM] * len(outs)),
        scratch_shapes=[pltpu.VMEM(shape, dtype) for shape, dtype in scratch],
        compiler_params=pltpu.CompilerParams(vmem_limit_bytes=20 << 20),
    )(*[pltpu.with_memory_space_constraint(x, pltpu.VMEM) for x in operands])


def enter_kernel(f_any, c_any, v_any, fh, fl, ch, cl, vt, g, f_buf, c_buf, v_buf, sems):
    n = c_buf.shape[0]
    per_part = ENTER_CHUNKS // 2
    rows = n // per_part
    v_copy = pltpu.make_async_copy(v_any, v_buf, sems.at[ENTER_CHUNKS])
    v_copy.start()
    copies = []
    places = [(i // per_part, pl.ds(i % per_part * rows, rows)) for i in range(ENTER_CHUNKS)]
    for i, place in enumerate(places):
        copies.append(pltpu.make_async_copy(f_any.at[place], f_buf.at[place], sems.at[i]))
        copies[-1].start()
    c_copy = pltpu.make_async_copy(c_any, c_buf, sems.at[ENTER_CHUNKS + 1])
    c_copy.start()
    v_copy.wait()
    real = v_buf[...]
    vt[...] = real
    pieces = []
    for copy, place in zip(copies, places):
        copy.wait()
        high, low = parts_of(f_buf[place])
        fh[place] = high
        fl[place] = low
        pieces.append(times(real, (high, low), NT))
    q = jnp.concatenate(pieces, axis=1)
    u = jnp.concatenate([q[:, :n], q[:, n:]], axis=0)
    c_copy.wait()
    write((ch, cl), c_buf[...])
    g[...] = times(u, read((ch, cl)), NN)


def only_on(layer, outs, compute):
    mine = lax.axis_index("row") // 2 == layer
    pl.when(mine)(compute)

    @pl.when(jnp.logical_not(mine))
    def _():
        for out in outs:
            out[...] = jnp.zeros_like(out)


def leave_kernel(*refs):
    only_on(0, refs[-2:], functools.partial(leave_body, *refs))


def leave_body(vt, g, fh, fl, ch, cl, lo, hi):
    y = add_real(g[...], vt[...])
    w = times(apply_to(y, tuple((fh[part], fl[part]) for part in range(2)), NT), read((ch, cl)), NN)
    half = lo.shape[0] // 2
    width = 2 * half
    lo[...] = jnp.concatenate([w[:half], w[width : width + half]], axis=0)
    hi[...] = jnp.concatenate([w[half:width], w[width + half :]], axis=0)


def pair_product(left, right, dims):
    return lax.dot_general(left[0], right[0], dims, preferred_element_type=F32) + (
        lax.dot_general(left[0], right[1], dims, preferred_element_type=F32)
        + lax.dot_general(left[1], right[0], dims, preferred_element_type=F32)
    )


def a_kernel(index, fh, fl, ch, cl, out):
    factor = (fh[index].T, fl[index].T)
    out[...] = pair_product(factor, read((ch, cl)), NN)


def b_kernel(fh, fl, ch, cl, out):
    couple = (ch[...].T, cl[...].T)
    for index in range(2):
        out[index] = pair_product(couple, (fh[index], fl[index]), NT)


def roles_kernel(count, *refs):
    sources = (refs[:count], refs[count : 2 * count])
    mats, buf, sems = refs[-3:]
    mine = lax.axis_index("row") % 2
    slots = (mine, 1 - mine)
    n = buf.shape[2]
    rows = n // (CHUNKS // 2)
    copies = []
    for side in range(2):
        halves = sources[side] if count == 2 else [sources[side][0].at[i] for i in range(2)]
        for index, half in enumerate(halves):
            for start in range(0, n, rows):
                part = pl.ds(start, rows)
                copy = pltpu.make_async_copy(
                    half.at[part], buf.at[side, index, part], sems.at[side, len(copies) % CHUNKS]
                )
                copy.start()
                copies.append((side, index, part, copy))
    for side, index, part, copy in copies:
        copy.wait()
        h, l = parts_of(buf[side, index, part, :])
        mats[0, slots[side], index, part, :] = h
        mats[1, slots[side], index, part, :] = l


def resident_roles_kernel(count, *refs):
    sources, mats = (refs[:count], refs[count : 2 * count]), refs[-1]
    mine = lax.axis_index("row") % 2
    for side, slot in enumerate((mine, 1 - mine)):
        for index in range(2):
            value = sources[side][index][...] if count == 2 else sources[side][0][index]
            mats[0, slot, index], mats[1, slot, index] = parts_of(value)


def roles_and_vectors_kernel(count, *refs):
    v_own, v_other, va, vb, mats = refs[2 * count :]
    resident_roles_kernel(count, *refs[: 2 * count], mats)
    mine = lax.axis_index("row") % 2
    half = va.shape[0]
    own = v_own[pl.ds(pl.multiple_of(mine * half, half), half), :]
    other = v_other[pl.ds(pl.multiple_of(mine * half, half), half), :]
    va[...] = jnp.where(mine == 0, own, other)
    vb[...] = jnp.where(mine == 0, other, own)


def resident_roles(owns, others, vectors=()):
    n = others[0].shape[-1]
    halves = [((v.shape[0] // 2, n), F32) for v in vectors]
    body = roles_and_vectors_kernel if vectors else resident_roles_kernel
    return call(
        functools.partial(body, len(others)),
        halves + [((2, 2, 2, n, n), BF16)],
        *owns, *others, *vectors,
    )


def roles(owns, others):
    n = others[0].shape[-1]
    shape = (2, 2, 2, n, n)
    return pl.pallas_call(
        functools.partial(roles_kernel, len(others)),
        out_shape=(pltpu.VMEM(shape, BF16),),
        in_specs=[HBM] * (2 * len(others)),
        out_specs=(VMEM,),
        scratch_shapes=[pltpu.VMEM(shape[1:], F32), pltpu.SemaphoreType.DMA((2, CHUNKS))],
        compiler_params=pltpu.CompilerParams(vmem_limit_bytes=20 << 20),
    )(*[pltpu.with_memory_space_constraint(x, pltpu.HBM) for x in owns], *others)


def total(refs):
    value = refs[0][...]
    for other in refs[1:]:
        value = value + other[...]
    return value


def forward_kernel(layer, *refs):
    only_on(layer, refs[-1:], functools.partial(forward_body, *refs))


def forward_body(*refs):
    *cs, va, vb, a_mats, out = refs
    y = apply_to(add_real(total(cs), va[...]), block_of(a_mats, 0), NN)
    out[...] = apply_to(add_real(y, vb[...]), block_of(a_mats, 1), NN)


def turn_kernel(*refs):
    *cs, va, vb, f_mats, a_mats, b_mats, ua, ub, s, weights = refs
    nodes = lax.axis_size("node")
    line = lax.broadcasted_iota(jnp.int32, weights.shape, 0)
    other, kind = line % nodes, line // nodes
    theta = 2.0 * math.pi * ((lax.axis_index("node") ^ other).astype(F32) + 0.5) / nodes
    angle = (kind // 2 + 1).astype(F32) * theta
    weights[...] = jnp.where(kind % 2 == 0, jnp.cos(angle), jnp.sin(angle)) / nodes
    y = add_real(total(cs), va[...])
    y_b = add_real(apply_to(y, block_of(a_mats, 0), NN), vb[...])
    u_b = apply_to(y_b, block_of(f_mats, 1), NT)
    u_a = apply_to(y, block_of(f_mats, 0), NT)
    ub[...] = u_b
    ua[...] = u_a
    s[...] = u_a + apply_to(u_b, block_of(b_mats, 0), NN)


def backward_kernel(layer, *refs):
    only_on(layer, refs[-1:], functools.partial(backward_body, *refs))


def backward_body(r, ua, ub, b_mats, xa):
    x_b = ub[...] + apply_to(r[...], block_of(b_mats, 1), NN)
    xa[...] = ua[...] + apply_to(x_b, block_of(b_mats, 0), NN)


def leave_backward_kernel(shares, *refs):
    *rs, ua, ub, b_mats = refs[: -1 - shares]
    *pieces, x = refs[-1 - shares :]
    node = lax.axis_index("node")
    x_b = ub[...] + apply_to(total(rs), block_of(b_mats, 1), NN)
    rows = x_b.shape[0]
    x[pl.ds(rows, rows), :] = x_b
    x[pl.ds(0, rows), :] = ua[...] + apply_to(x_b, block_of(b_mats, 0), NN)
    for d, piece in enumerate(pieces):
        lanes = piece.shape[1]
        piece[...] = x[:, pl.ds(pl.multiple_of((node ^ d) * lanes, lanes), lanes)]


def combine_kernel(*refs):
    *pieces, weights, out = refs
    nodes = len(pieces)
    half = pieces[0].shape[0] // 4
    share = out.shape[1]
    groups = 2 * MOM
    for b in range(2):
        parts = [
            [piece[pl.ds((2 * b + part) * half, half), :] for piece in pieces] for part in range(2)
        ]
        for order in range(MOM):
            w_re, w_im = (
                [weights[pl.ds((2 * order + part) * nodes + d, 1), :][:, :share] for d in range(nodes)]
                for part in range(2)
            )
            re = [w_re[d] * parts[0][d] - w_im[d] * parts[1][d] for d in range(nodes)]
            im = [w_re[d] * parts[1][d] + w_im[d] * parts[0][d] for d in range(nodes)]
            row = (b * groups + 2 * order) * half
            out[pl.ds(row, half), :] = tree_sum(re)
            out[pl.ds(row + half, half), :] = tree_sum(im)


def gram_kernel(mine, other, moments, *outs):
    *owns, buf = outs
    node = lax.axis_index("node")
    first = lax.axis_index("row") % 2 == 0
    groups = 2 * MOM
    half = mine.shape[0] // (2 * groups)
    gram, both = None, []
    for b in range(2):
        part = pl.ds(b * groups * half, groups * half)
        a, o = mine[part, :], other[part, :]
        lo, hi = jnp.where(first, a, o), jnp.where(first, o, a)
        cuts = [slice(g * half, (g + 1) * half) for g in range(groups)]
        both.append(jnp.concatenate([side[cut] for cut in cuts for side in (lo, hi)], axis=0))
        product = times(a, parts_of(both[b]), NT)
        gram = product if gram is None else gram + product
    buf[...] = gram
    for d, own in enumerate(owns):
        rows = own.shape[0]
        own[...] = buf[pl.ds(pl.multiple_of((node ^ d) * rows, rows), rows), :]
    moments[...] = jnp.where(first, both[0], both[1])


def gather_kernel(*refs):
    *pieces, out = refs
    node = lax.axis_index("node")
    for d, piece in enumerate(pieces):
        rows = piece.shape[0]
        out[pl.ds(pl.multiple_of((node ^ d) * rows, rows), rows), :] = piece[...]


def join_kernel(mine, other, out):
    first = lax.axis_index("row") % 2 == 0
    groups = 2 * MOM
    half = mine.shape[0] // groups
    for g in range(groups):
        cut = pl.ds(g * half, half)
        out[pl.ds(2 * g * half, half), :] = jnp.where(first, mine[cut, :], other[cut, :])
        out[pl.ds((2 * g + 1) * half, half), :] = jnp.where(first, other[cut, :], mine[cut, :])


def after(*values, every=False):
    held = lax.optimization_barrier(values)
    return held if every else held[0]


def tree_sum(values):
    while len(values) > 1:
        values = [values[i] + values[i + 1] for i in range(0, len(values), 2)]
    return values[0]


def shards(inv_factors, coupling, vectors):
    n = inv_factors.shape[3]
    width = vectors.shape[2]
    half = width // 2
    rows = lax.axis_size("row")
    nodes = lax.axis_size("node")
    layers = rows // 2

    def swap_core(value):
        return lax.ppermute(value, "row", [(r, r ^ 1) for r in range(rows)])

    def hop(value, source, target):
        return lax.ppermute(value, "row", [(2 * source + c, 2 * target + c) for c in range(2)])

    def exchange_node(value, d):
        return lax.ppermute(value, "node", [(j, j ^ d) for j in range(nodes)])

    def exchange_layer(value, d):
        return lax.ppermute(value, "row", [(r, r ^ (2 * d)) for r in range(rows)])

    factor = inv_factors[0, 0]
    couple = coupling[0]
    block = ((2 * half, n), F32)

    fh, fl, ch, cl, v_t, g = pl.pallas_call(
        enter_kernel,
        out_shape=(
            pltpu.VMEM((2, n, n), BF16),
            pltpu.VMEM((2, n, n), BF16),
            pltpu.VMEM((n, n), BF16),
            pltpu.VMEM((n, n), BF16),
            pltpu.VMEM((width, n), F32),
            pltpu.VMEM((2 * width, n), F32),
        ),
        in_specs=[HBM] * 3,
        out_specs=(VMEM,) * 6,
        scratch_shapes=[
            pltpu.VMEM((2, n, n), F32),
            pltpu.VMEM((n, n), F32),
            pltpu.VMEM((width, n), F32),
            pltpu.SemaphoreType.DMA((ENTER_CHUNKS + 2,)),
        ],
        compiler_params=pltpu.CompilerParams(vmem_limit_bytes=20 << 20),
        name="enter",
    )(*[pltpu.with_memory_space_constraint(x, pltpu.HBM) for x in (factor, couple, vectors[0].T)])
    from_a = swap_core(g)
    (a_re,) = call(functools.partial(a_kernel, 0), [((n, n), F32)], after(fh, g), fl, ch, cl)
    lo, hi = call(leave_kernel, [block, block], v_t, from_a, after(fh, from_a), fl, ch, cl)

    got_lo = lax.ppermute(lo, "row", [(1, 2)])
    got_hi = lax.ppermute(hi, "row", [(1, 3)])
    got = [got_lo, got_hi]
    (a_im,) = call(functools.partial(a_kernel, 1), [((n, n), F32)], after(fh, lo), fl, ch, cl)
    a_re_other = swap_core(after(a_re, from_a))
    a_im_other = swap_core(a_im)
    v_other = swap_core(after(v_t, lo))
    va, vb, a_mats = resident_roles([a_re, a_im], [a_re_other, a_im_other], [v_t, v_other])
    f_other = swap_core(after(factor, a_re_other, a_im_other))
    arrived = []
    for t in range(layers - 1):
        if t > 0:
            got = [hop(leaving, t, t + 1)]
        arrived += got
        if t < layers - 2:
            (leaving,) = call(
                functools.partial(forward_kernel, t + 1), [block], *got, va, vb, a_mats
            )
        if t == 0:
            (f_mats,) = roles([after(factor, leaving)], [f_other])
            (b_own,) = call(b_kernel, [((2, n, n), F32)], after(fh, leaving), fl, ch, cl)
            b_other = swap_core(b_own)
        if t == 1:
            (b_mats,) = resident_roles([after(b_own, leaving, f_mats)], [b_other])
    u_a, u_b, leaving, weights = call(
        turn_kernel, [block] * 3 + [((2 * MOM * nodes, 128), F32)], *arrived, va, vb, f_mats, a_mats, b_mats
    )

    arrived = []
    for t in range(layers - 1, 0, -1):
        got = hop(leaving, t, t - 1)
        arrived.append(got)
        if t > 1:
            (leaving,) = call(
                functools.partial(backward_kernel, t - 1), [block], got, u_a, u_b, b_mats
            )
    share = n // nodes
    shares = nodes if share % 128 == 0 else 0
    x_both = ((4 * half, n), F32)
    pieces = call(
        functools.partial(leave_backward_kernel, shares),
        [((4 * half, share), F32)] * shares or [x_both],
        *arrived, u_a, u_b, b_mats,
        scratch=[x_both] if shares else [],
    )

    if not shares:
        node = lax.axis_index("node")
        pieces = [
            lax.dynamic_slice_in_dim(pieces[0], (node ^ d) * share, share, 1)
            for d in range(nodes)
        ]
    pieces = [pieces[0]] + [exchange_node(pieces[d], d) for d in range(1, nodes)]
    groups = 2 * MOM
    cols = groups * width
    (mine,) = call(combine_kernel, [((2 * groups * half, share), F32)], *pieces, weights)
    other = swap_core(mine)

    hc = groups * half
    gs = hc // nodes
    moments, *own = call(
        gram_kernel,
        [((cols, share), F32)] + [((gs, cols), F32)] * nodes,
        mine, other,
        scratch=[((hc, cols), F32)],
    )
    piece = tree_sum([own[0]] + [exchange_node(own[d], d) for d in range(1, nodes)])
    piece = tree_sum([piece] + [exchange_layer(piece, d) for d in range(1, layers)])
    piece = piece * (nodes / (rows * n))
    got = [piece] + [exchange_node(piece, d) for d in range(1, nodes)]
    (gram,) = call(gather_kernel, [((hc, cols), F32)], *got)
    other = swap_core(gram)
    gram = pl.pallas_call(
        join_kernel,
        out_shape=jax.ShapeDtypeStruct((cols, cols), F32),
        in_specs=[VMEM] * 2,
        out_specs=VMEM,
        compiler_params=pltpu.CompilerParams(vmem_limit_bytes=20 << 20),
        name="join",
    )(*[pltpu.with_memory_space_constraint(x, pltpu.VMEM) for x in (gram, other)])
    return moments.T[None], gram


def solution(mesh):
    return jax.shard_map(
        shards,
        mesh=mesh,
        in_specs=(
            P(("intv", "node"), "row", None, None, None),
            P("row", None, None),
            P("row", None, None),
        ),
        out_specs=(P(("intv", "row"), "node", None), P("intv", None)),
        check_vma=False,
    )
```

```python
import functools
import functools
import math

import jax
import jax.numpy as jnp
from jax import lax
from jax.experimental import pallas as pl
from jax.experimental.pallas import tpu as pltpu
from jax.sharding import PartitionSpec as P


MOM = 2
F32, BF16 = jnp.float32, jnp.bfloat16
NN = (((1,), (0,)), ((), ()))
NT = (((1,), (1,)), ((), ()))
VMEM = pl.BlockSpec(memory_space=pltpu.VMEM)
HBM = pl.BlockSpec(memory_space=pltpu.HBM)
CHUNKS = 4
ENTER_CHUNKS = 2


def parts_of(x):
    high = x.astype(BF16)
    return high, (x - high.astype(F32)).astype(BF16)


def times(rows, matrix, dims):
    w = rows.shape[0]
    high, low = parts_of(rows)
    both = lax.dot_general(
        jnp.concatenate([high, low], axis=0), matrix[0], dims, preferred_element_type=F32
    )
    rest = lax.dot_general(high, matrix[1], dims, preferred_element_type=F32)
    return both[:w] + (both[w:] + rest)


def apply_to(rows, matrix, dims):
    w = rows.shape[0] // 2
    re, im = (times(rows, part, dims) for part in matrix)
    return jnp.concatenate([re[:w] - im[w:], im[:w] + re[w:]], axis=0)


def add_real(block, real):
    w = real.shape[0]
    return jnp.concatenate([block[:w] + real, block[w:]], axis=0)


def read(pair):
    return pair[0][...], pair[1][...]


def block_of(mats, role):
    return tuple((mats[0, role, part], mats[1, role, part]) for part in range(2))


def write(pair, value):
    high, low = parts_of(value)
    pair[0][...] = high
    pair[1][...] = low


def call(kernel, outs, *operands, scratch=()):
    return pl.pallas_call(
        kernel,
        out_shape=tuple(pltpu.VMEM(shape, dtype) for shape, dtype in outs),
        in_specs=[VMEM] * len(operands),
        out_specs=tuple([VMEM] * len(outs)),
        scratch_shapes=[pltpu.VMEM(shape, dtype) for shape, dtype in scratch],
        compiler_params=pltpu.CompilerParams(vmem_limit_bytes=20 << 20),
    )(*[pltpu.with_memory_space_constraint(x, pltpu.VMEM) for x in operands])


def enter_kernel(f_any, c_any, v_any, fh, fl, ch, cl, vt, g, f_buf, c_buf, v_buf, sems):
    n = c_buf.shape[0]
    per_part = ENTER_CHUNKS // 2
    rows = n // per_part
    v_copy = pltpu.make_async_copy(v_any, v_buf, sems.at[ENTER_CHUNKS])
    v_copy.start()
    copies = []
    places = [(i // per_part, pl.ds(i % per_part * rows, rows)) for i in range(ENTER_CHUNKS)]
    for i, place in enumerate(places):
        copies.append(pltpu.make_async_copy(f_any.at[place], f_buf.at[place], sems.at[i]))
        copies[-1].start()
    c_copy = pltpu.make_async_copy(c_any, c_buf, sems.at[ENTER_CHUNKS + 1])
    c_copy.start()
    v_copy.wait()
    real = v_buf[...]
    vt[...] = real
    pieces = []
    for copy, place in zip(copies, places):
        copy.wait()
        high, low = parts_of(f_buf[place])
        fh[place] = high
        fl[place] = low
        pieces.append(times(real, (high, low), NT))
    q = jnp.concatenate(pieces, axis=1)
    u = jnp.concatenate([q[:, :n], q[:, n:]], axis=0)
    c_copy.wait()
    write((ch, cl), c_buf[...])
    g[...] = times(u, read((ch, cl)), NN)


def only_on(layer, outs, compute):
    mine = lax.axis_index("row") // 2 == layer
    pl.when(mine)(compute)

    @pl.when(jnp.logical_not(mine))
    def _():
        for out in outs:
            out[...] = jnp.zeros_like(out)


def leave_kernel(*refs):
    only_on(0, refs[-2:], functools.partial(leave_body, *refs))


def leave_body(vt, g, fh, fl, ch, cl, lo, hi):
    y = add_real(g[...], vt[...])
    w = times(apply_to(y, tuple((fh[part], fl[part]) for part in range(2)), NT), read((ch, cl)), NN)
    half = lo.shape[0] // 2
    width = 2 * half
    lo[...] = jnp.concatenate([w[:half], w[width : width + half]], axis=0)
    hi[...] = jnp.concatenate([w[half:width], w[width + half :]], axis=0)


def pair_product(left, right, dims):
    return lax.dot_general(left[0], right[0], dims, preferred_element_type=F32) + (
        lax.dot_general(left[0], right[1], dims, preferred_element_type=F32)
        + lax.dot_general(left[1], right[0], dims, preferred_element_type=F32)
    )


def a_kernel(index, fh, fl, ch, cl, out):
    factor = (fh[index].T, fl[index].T)
    out[...] = pair_product(factor, read((ch, cl)), NN)


def b_kernel(fh, fl, ch, cl, out):
    couple = (ch[...].T, cl[...].T)
    for index in range(2):
        out[index] = pair_product(couple, (fh[index], fl[index]), NT)


def roles_kernel(count, *refs):
    sources = (refs[:count], refs[count : 2 * count])
    mats, buf, sems = refs[-3:]
    mine = lax.axis_index("row") % 2
    slots = (mine, 1 - mine)
    n = buf.shape[2]
    rows = n // (CHUNKS // 2)
    copies = []
    for side in range(2):
        halves = sources[side] if count == 2 else [sources[side][0].at[i] for i in range(2)]
        for index, half in enumerate(halves):
            for start in range(0, n, rows):
                part = pl.ds(start, rows)
                copy = pltpu.make_async_copy(
                    half.at[part], buf.at[side, index, part], sems.at[side, len(copies) % CHUNKS]
                )
                copy.start()
                copies.append((side, index, part, copy))
    for side, index, part, copy in copies:
        copy.wait()
        h, l = parts_of(buf[side, index, part, :])
        mats[0, slots[side], index, part, :] = h
        mats[1, slots[side], index, part, :] = l


def resident_roles_kernel(count, *refs):
    sources, mats = (refs[:count], refs[count : 2 * count]), refs[-1]
    mine = lax.axis_index("row") % 2
    for side, slot in enumerate((mine, 1 - mine)):
        for index in range(2):
            value = sources[side][index][...] if count == 2 else sources[side][0][index]
            mats[0, slot, index], mats[1, slot, index] = parts_of(value)


def roles_and_vectors_kernel(count, *refs):
    v_own, v_other, va, vb, mats = refs[2 * count :]
    resident_roles_kernel(count, *refs[: 2 * count], mats)
    mine = lax.axis_index("row") % 2
    half = va.shape[0]
    own = v_own[pl.ds(pl.multiple_of(mine * half, half), half), :]
    other = v_other[pl.ds(pl.multiple_of(mine * half, half), half), :]
    va[...] = jnp.where(mine == 0, own, other)
    vb[...] = jnp.where(mine == 0, other, own)


def resident_roles(owns, others, vectors=()):
    n = others[0].shape[-1]
    halves = [((v.shape[0] // 2, n), F32) for v in vectors]
    body = roles_and_vectors_kernel if vectors else resident_roles_kernel
    return call(
        functools.partial(body, len(others)),
        halves + [((2, 2, 2, n, n), BF16)],
        *owns, *others, *vectors,
    )


def roles(owns, others):
    n = others[0].shape[-1]
    shape = (2, 2, 2, n, n)
    return pl.pallas_call(
        functools.partial(roles_kernel, len(others)),
        out_shape=(pltpu.VMEM(shape, BF16),),
        in_specs=[HBM] * (2 * len(others)),
        out_specs=(VMEM,),
        scratch_shapes=[pltpu.VMEM(shape[1:], F32), pltpu.SemaphoreType.DMA((2, CHUNKS))],
        compiler_params=pltpu.CompilerParams(vmem_limit_bytes=20 << 20),
    )(*[pltpu.with_memory_space_constraint(x, pltpu.HBM) for x in owns], *others)


def total(refs):
    value = refs[0][...]
    for other in refs[1:]:
        value = value + other[...]
    return value


def forward_kernel(layer, *refs):
    only_on(layer, refs[-1:], functools.partial(forward_body, *refs))


def forward_body(*refs):
    *cs, va, vb, a_mats, out = refs
    y = apply_to(add_real(total(cs), va[...]), block_of(a_mats, 0), NN)
    out[...] = apply_to(add_real(y, vb[...]), block_of(a_mats, 1), NN)


def turn_kernel(*refs):
    *cs, va, vb, f_mats, a_mats, b_mats, ua, ub, s, weights = refs
    nodes = lax.axis_size("node")
    line = lax.broadcasted_iota(jnp.int32, weights.shape, 0)
    other, kind = line % nodes, line // nodes
    theta = 2.0 * math.pi * ((lax.axis_index("node") ^ other).astype(F32) + 0.5) / nodes
    angle = (kind // 2 + 1).astype(F32) * theta
    weights[...] = jnp.where(kind % 2 == 0, jnp.cos(angle), jnp.sin(angle)) / nodes
    y = add_real(total(cs), va[...])
    a_y = apply_to(y, block_of(a_mats, 0), NN)
    u_a = apply_to(y, block_of(f_mats, 0), NT)
    u_b = apply_to(add_real(a_y, vb[...]), block_of(f_mats, 1), NT)
    ub[...] = u_b
    ua[...] = u_a

    def send():
        s[...] = u_a + apply_to(ub[...], block_of(b_mats, 0), NN)

    only_on(lax.axis_size("row") // 2 - 1, [s], send)


def backward_kernel(layer, *refs):
    only_on(layer, refs[-1:], functools.partial(backward_body, *refs))


def backward_body(r, ua, ub, b_mats, xa):
    x_b = ub[...] + apply_to(r[...], block_of(b_mats, 1), NN)
    xa[...] = ua[...] + apply_to(x_b, block_of(b_mats, 0), NN)


def leave_backward_kernel(shares, *refs):
    *rs, ua, ub, b_mats = refs[: -1 - shares]
    *pieces, x = refs[-1 - shares :]
    node = lax.axis_index("node")
    x_b = ub[...] + apply_to(total(rs), block_of(b_mats, 1), NN)
    rows = x_b.shape[0]
    x[pl.ds(rows, rows), :] = x_b
    x[pl.ds(0, rows), :] = ua[...] + apply_to(x_b, block_of(b_mats, 0), NN)
    for d, piece in enumerate(pieces):
        lanes = piece.shape[1]
        piece[...] = x[:, pl.ds(pl.multiple_of((node ^ d) * lanes, lanes), lanes)]


def combine_kernel(*refs):
    *pieces, weights, out = refs
    nodes = len(pieces)
    half = pieces[0].shape[0] // 4
    share = out.shape[1]
    groups = 2 * MOM
    for b in range(2):
        parts = [
            [piece[pl.ds((2 * b + part) * half, half), :] for piece in pieces] for part in range(2)
        ]
        for order in range(MOM):
            w_re, w_im = (
                [weights[pl.ds((2 * order + part) * nodes + d, 1), :][:, :share] for d in range(nodes)]
                for part in range(2)
            )
            re = [w_re[d] * parts[0][d] - w_im[d] * parts[1][d] for d in range(nodes)]
            im = [w_re[d] * parts[1][d] + w_im[d] * parts[0][d] for d in range(nodes)]
            row = (b * groups + 2 * order) * half
            out[pl.ds(row, half), :] = tree_sum(re)
            out[pl.ds(row + half, half), :] = tree_sum(im)


def gram_kernel(mine, other, moments, *outs):
    *owns, buf = outs
    node = lax.axis_index("node")
    first = lax.axis_index("row") % 2 == 0
    groups = 2 * MOM
    half = mine.shape[0] // (2 * groups)
    gram, both = None, []
    for b in range(2):
        part = pl.ds(b * groups * half, groups * half)
        a, o = mine[part, :], other[part, :]
        lo, hi = jnp.where(first, a, o), jnp.where(first, o, a)
        cuts = [slice(g * half, (g + 1) * half) for g in range(groups)]
        both.append(jnp.concatenate([side[cut] for cut in cuts for side in (lo, hi)], axis=0))
        product = times(a, parts_of(both[b]), NT)
        gram = product if gram is None else gram + product
    buf[...] = gram
    for d, own in enumerate(owns):
        rows = own.shape[0]
        own[...] = buf[pl.ds(pl.multiple_of((node ^ d) * rows, rows), rows), :]
    moments[...] = jnp.where(first, both[0], both[1])


def gather_kernel(*refs):
    *pieces, out = refs
    node = lax.axis_index("node")
    for d, piece in enumerate(pieces):
        rows = piece.shape[0]
        out[pl.ds(pl.multiple_of((node ^ d) * rows, rows), rows), :] = piece[...]


def join_kernel(mine, other, out):
    first = lax.axis_index("row") % 2 == 0
    groups = 2 * MOM
    half = mine.shape[0] // groups
    for g in range(groups):
        cut = pl.ds(g * half, half)
        out[pl.ds(2 * g * half, half), :] = jnp.where(first, mine[cut, :], other[cut, :])
        out[pl.ds((2 * g + 1) * half, half), :] = jnp.where(first, other[cut, :], mine[cut, :])


def after(*values, every=False):
    held = lax.optimization_barrier(values)
    return held if every else held[0]


def tree_sum(values):
    while len(values) > 1:
        values = [values[i] + values[i + 1] for i in range(0, len(values), 2)]
    return values[0]


def shards(inv_factors, coupling, vectors):
    n = inv_factors.shape[3]
    width = vectors.shape[2]
    half = width // 2
    rows = lax.axis_size("row")
    nodes = lax.axis_size("node")
    layers = rows // 2

    def swap_core(value):
        return lax.ppermute(value, "row", [(r, r ^ 1) for r in range(rows)])

    def hop(value, source, target):
        return lax.ppermute(value, "row", [(2 * source + c, 2 * target + c) for c in range(2)])

    def exchange_node(value, d):
        return lax.ppermute(value, "node", [(j, j ^ d) for j in range(nodes)])

    def exchange_layer(value, d):
        return lax.ppermute(value, "row", [(r, r ^ (2 * d)) for r in range(rows)])

    factor = inv_factors[0, 0]
    couple = coupling[0]
    block = ((2 * half, n), F32)

    fh, fl, ch, cl, v_t, g = pl.pallas_call(
        enter_kernel,
        out_shape=(
            pltpu.VMEM((2, n, n), BF16),
            pltpu.VMEM((2, n, n), BF16),
            pltpu.VMEM((n, n), BF16),
            pltpu.VMEM((n, n), BF16),
            pltpu.VMEM((width, n), F32),
            pltpu.VMEM((2 * width, n), F32),
        ),
        in_specs=[HBM] * 3,
        out_specs=(VMEM,) * 6,
        scratch_shapes=[
            pltpu.VMEM((2, n, n), F32),
            pltpu.VMEM((n, n), F32),
            pltpu.VMEM((width, n), F32),
            pltpu.SemaphoreType.DMA((ENTER_CHUNKS + 2,)),
        ],
        compiler_params=pltpu.CompilerParams(vmem_limit_bytes=20 << 20),
        name="enter",
    )(*[pltpu.with_memory_space_constraint(x, pltpu.HBM) for x in (factor, couple, vectors[0].T)])
    from_a = swap_core(g)
    (a_re,) = call(functools.partial(a_kernel, 0), [((n, n), F32)], after(fh, g), fl, ch, cl)
    lo, hi = call(leave_kernel, [block, block], v_t, from_a, after(fh, from_a), fl, ch, cl)

    got_lo = lax.ppermute(lo, "row", [(1, 2)])
    got_hi = lax.ppermute(hi, "row", [(1, 3)])
    got = [got_lo, got_hi]
    (a_im,) = call(functools.partial(a_kernel, 1), [((n, n), F32)], after(fh, lo), fl, ch, cl)
    a_re_other = swap_core(after(a_re, from_a))
    a_im_other = swap_core(a_im)
    v_other = swap_core(after(v_t, lo))
    va, vb, a_mats = resident_roles([a_re, a_im], [a_re_other, a_im_other], [v_t, v_other])
    f_other = swap_core(after(factor, a_re_other, a_im_other))
    arrived = []
    for t in range(layers - 1):
        if t > 0:
            got = [hop(leaving, t, t + 1)]
        arrived += got
        if t < layers - 2:
            (leaving,) = call(
                functools.partial(forward_kernel, t + 1), [block], *got, va, vb, a_mats
            )
        if t == 0:
            (f_mats,) = roles([after(factor, leaving)], [f_other])
            (b_own,) = call(b_kernel, [((2, n, n), F32)], after(fh, leaving), fl, ch, cl)
            b_other = swap_core(b_own)
        if t == 1:
            (b_mats,) = resident_roles([after(b_own, leaving, f_mats)], [b_other])
    u_a, u_b, leaving, weights = call(
        turn_kernel, [block] * 3 + [((2 * MOM * nodes, 128), F32)], *arrived, va, vb, f_mats, a_mats, b_mats
    )

    arrived = []
    for t in range(layers - 1, 0, -1):
        got = hop(leaving, t, t - 1)
        arrived.append(got)
        if t > 1:
            (leaving,) = call(
                functools.partial(backward_kernel, t - 1), [block], got, u_a, u_b, b_mats
            )
    share = n // nodes
    shares = nodes if share % 128 == 0 else 0
    x_both = ((4 * half, n), F32)
    pieces = call(
        functools.partial(leave_backward_kernel, shares),
        [((4 * half, share), F32)] * shares or [x_both],
        *arrived, u_a, u_b, b_mats,
        scratch=[x_both] if shares else [],
    )

    if not shares:
        node = lax.axis_index("node")
        pieces = [
            lax.dynamic_slice_in_dim(pieces[0], (node ^ d) * share, share, 1)
            for d in range(nodes)
        ]
    pieces = [pieces[0]] + [exchange_node(pieces[d], d) for d in range(1, nodes)]
    groups = 2 * MOM
    cols = groups * width
    (mine,) = call(combine_kernel, [((2 * groups * half, share), F32)], *pieces, weights)
    other = swap_core(mine)

    hc = groups * half
    gs = hc // nodes
    moments, *own = call(
        gram_kernel,
        [((cols, share), F32)] + [((gs, cols), F32)] * nodes,
        mine, other,
        scratch=[((hc, cols), F32)],
    )
    piece = tree_sum([own[0]] + [exchange_node(own[d], d) for d in range(1, nodes)])
    piece = tree_sum([piece] + [exchange_layer(piece, d) for d in range(1, layers)])
    piece = piece * (nodes / (rows * n))
    got = [piece] + [exchange_node(piece, d) for d in range(1, nodes)]
    (gram,) = call(gather_kernel, [((hc, cols), F32)], *got)
    other = swap_core(gram)
    gram = pl.pallas_call(
        join_kernel,
        out_shape=jax.ShapeDtypeStruct((cols, cols), F32),
        in_specs=[VMEM] * 2,
        out_specs=VMEM,
        compiler_params=pltpu.CompilerParams(vmem_limit_bytes=20 << 20),
        name="join",
    )(*[pltpu.with_memory_space_constraint(x, pltpu.VMEM) for x in (gram, other)])
    return moments.T[None], gram


def solution(mesh):
    return jax.shard_map(
        shards,
        mesh=mesh,
        in_specs=(
            P(("intv", "node"), "row", None, None, None),
            P("row", None, None),
            P("row", None, None),
        ),
        out_specs=(P(("intv", "row"), "node", None), P("intv", None)),
        check_vma=False,
    )
```
